128 devices in a mesh: up: 16 (over y_lo, x, core), dn: 8 (over y_hi, z).
Axes of the slice: x: 4, y: 4 (y_hi: 2, y_lo: 2; y = y_hi * 2 + y_lo), z: 4, core: 2. Of those that a mesh axis runs over, the one named last changes fastest.
Arguments:
- start_vector: bfloat16 [13312, 13312], P('up', 'dn'), may hold values from -6 to 6
- hop_tiles: bfloat16 [104, 5, 128, 128], replicated, may hold values from -0.5 to 0.5
- tile_columns: int32 [104, 5], replicated, may hold values from 0 to 103, as said below
- tile_signs: int32 [104, 5], replicated, may hold values from 0 to 1
- occupation: int32 [16, 13312], replicated, may hold values from 0 to 1, as said below
Outputs:
- next_vector: bfloat16 [13312, 13312], P('up', 'dn')
- alphas: float32 [2], replicated
- betas: float32 [2], replicated
The draws below stay inside these ranges and needn't reach their ends.
Inputs may be any that keep to these rules, and one draw needn't show every extreme that they name: Each row of tile_columns names 5 different tile columns. Every column of occupation holds exactly 8 ones.
All inputs are finite; a program needn't handle non-finite values.
Results may differ from the reference program's by a relative error of at most 0.0065.
Values may be sent and summed in bfloat16 or wider, within the bound.
A program may use at most 192 MiB of HBM per device.

```python
import jax
import jax.numpy as jnp
from jax import lax

DETS = 13312
SITES = 16
TILE = 128
TILE_K = 5
STEPS = 2
TILES = 104


def draw_tile_columns(key, part):
    scores = jax.random.randint(key, (TILES, TILES), 0, 1 << 20) * TILES + jnp.arange(TILES, dtype=jnp.int32)[None, :]
    order = jnp.argsort(scores, axis=1)
    return order[:, :TILE_K].astype(jnp.int32)


def draw_occupation(key, part):
    scores = jax.random.randint(key, (DETS, SITES), 0, 1 << 20) * SITES + jnp.arange(SITES, dtype=jnp.int32)[None, :]
    ranks = jnp.argsort(jnp.argsort(scores, axis=1), axis=1)
    filled = (ranks < SITES // 2).astype(jnp.int32)
    return filled.T


def with_ends(drawn, key, smallest, high):
    dims = drawn.shape
    index_at = [jax.random.randint(jax.random.fold_in(key, axis), (), 0, dims[axis]) for axis in range(len(dims))]
    drawn = drawn.at[tuple(index_at)].set(smallest)
    longest = dims.index(max(dims))
    index_at[longest] = (index_at[longest] + 1) % dims[longest]
    return drawn.at[tuple(index_at)].set(high)


def block_scale(key, dims, shards, smallest, high):
    level = 1.0
    for dim, blocks in shards:
        draws = jax.random.uniform(jax.random.fold_in(jax.random.fold_in(key, 6), dim), (blocks,), jnp.float32, smallest / len(shards), high / len(shards))
        level = level * jnp.repeat(jnp.exp(draws), dims[dim] // blocks).reshape((-1,) + (1,) * (len(dims) - 1 - dim))
    return level


def bell_draw(rng, shape, spread, most, pieces=(), held_as=jnp.bfloat16):
    loudness = block_scale(rng, shape, pieces, -0.22, 0.18) if pieces else 1.0
    entries = jax.random.normal(rng, shape, jnp.float32) * spread * loudness
    return jnp.minimum(jnp.maximum(entries, -most), most).astype(held_as)


def setup_inputs(seed: int = 0) -> dict:
    seeds = jax.random.split(jax.random.key(seed), 6)
    start_vector = bell_draw(seeds[0], (DETS, DETS), 1.0, 6.0, ((0, 16), (1, 8)))
    hop_tiles = bell_draw(seeds[1], (TILES, TILE_K, TILE, TILE), TILE ** -0.5, 0.5)
    tile_columns = draw_tile_columns(jax.random.fold_in(seeds[5], 71), 0)
    tile_signs = with_ends(jax.random.randint(seeds[3], (TILES, TILE_K), 0, 2), jax.random.fold_in(seeds[3], 1), 0, 1).astype(jnp.int32)
    occupation = draw_occupation(jax.random.fold_in(seeds[5], 71), 0)
    return {"start_vector": start_vector, "hop_tiles": hop_tiles, "tile_columns": tile_columns, "tile_signs": tile_signs, "occupation": occupation}


coupling = 4.0

def hop_last(matrix, signed_wide, tile_columns):

    def one_block(part):
        cube = part.reshape(part.shape[0], TILES, TILE)
        picked = cube[:, tile_columns].astype(jnp.float32)
        result = jnp.einsum('ikab,mikb->mia', signed_wide, picked, precision=lax.Precision.HIGHEST)
        return result.reshape(part.shape)
    blocks = matrix.reshape(-1, 512, matrix.shape[1])
    return lax.map(one_block, blocks).reshape(matrix.shape)

def reference(start_vector, hop_tiles, tile_columns, tile_signs, occupation):
    signed = hop_tiles * (1 - 2 * tile_signs).astype(jnp.bfloat16)[:, :, None, None]
    signed_wide = signed.astype(jnp.float32)
    occupied = occupation.astype(jnp.bfloat16)
    diagonal = coupling * jnp.dot(occupied.T, occupied, preferred_element_type=jnp.float32)
    vector = start_vector.astype(jnp.float32)
    total = jnp.sum(vector * vector)
    vector = vector / jnp.maximum(jnp.sqrt(total), 1.0)
    previous = jnp.zeros_like(vector)
    beta_value = jnp.float32(0.0)
    alpha_list = []
    beta_list = []
    for iteration in range(STEPS):
        rounded = vector.astype(jnp.bfloat16)
        hopped_up = hop_last(rounded.T, signed_wide, tile_columns).T.astype(jnp.bfloat16)
        hopped_down = hop_last(rounded, signed_wide, tile_columns).astype(jnp.bfloat16)
        work = hopped_up.astype(jnp.float32) + hopped_down.astype(jnp.float32) + diagonal * vector - beta_value * previous
        intersect = jnp.sum(work * vector)
        work = work - intersect * vector
        residual = jnp.sum(work * work)
        beta_value = jnp.sqrt(jnp.maximum(residual, 1.0))
        previous = vector
        vector = work / beta_value
        alpha_list.append(intersect)
        beta_list.append(beta_value)
    return (vector.astype(jnp.bfloat16), jnp.stack(alpha_list), jnp.stack(beta_list))
```

```python
import functools

import jax
import jax.numpy as jnp
from jax import lax
from jax.experimental import pallas as pl
from jax.experimental.pallas import tpu as pltpu
from jax.sharding import PartitionSpec as P

STEPS = 2
RING = 4
TILE = 128
MESH = pl.DeviceIdType.MESH

coupling = 4.0


def place():
    u = lax.axis_index("up")
    d = lax.axis_index("dn")
    return u // 8, (u // 2) % 4, u % 2, d // 4, d % 4


def device(y_lo, x, core, y_hi, z):
    return (y_lo * 8 + x * 2 + core, y_hi * 4 + z)


def turn(source, target, side):
    tiles = side // TILE

    def one_row(i, carry):
        at = pl.multiple_of(i * TILE, TILE)
        for j in range(tiles):
            target[i, j * TILE : (j + 1) * TILE, :] = source[j, pl.ds(at, TILE), :].T
        return carry

    lax.fori_loop(0, tiles, one_row, 0)


def exchange_kernel(
    tile_k,
    columns_ref,
    signs_ref,
    x_ref,
    tiles_ref,
    mine_ref,
    other_ref,
    own,
    near,
    far,
    turned,
    turned_near,
    gathered,
    result,
    returned,
    weights,
    load_sem,
    tiles_sem,
    sib_send,
    sib_recv,
    near_send,
    near_recv,
    far_send,
    far_recv,
    share_send,
    share_recv,
    ring_send,
    ring_recv,
    back_send,
    back_recv,
    last_send,
    last_recv,
):
    half = x_ref.shape[0]
    side = 2 * half
    quarter = side // RING
    chunks = near_send.shape[0]
    step = half // chunks
    per_piece = side // TILE
    held = RING * per_piece
    y_lo, x, core, y_hi, z = place()
    r = z + core * (x - z)
    h = y_hi + core * (y_lo - y_hi)
    sibling = device(y_lo, x, 1 - core, y_hi, z)
    near_chip = device(1 - y_lo, x, core, y_hi, z)
    far_chip = device(1 - y_lo, x, core, 1 - y_hi, z)

    def ring_peer(p):
        return device(y_lo, x + core * (p - x), core, y_hi, p + core * (z - p))

    def remote(src, dst, send, recv, to):
        return pltpu.make_async_remote_copy(
            src_ref=src, dst_ref=dst, send_sem=send, recv_sem=recv, device_id=to, device_id_type=MESH
        )

    barrier = pltpu.get_barrier_semaphore()
    greeted = [sibling, near_chip, far_chip] + [ring_peer((r + k) % RING) for k in range(1, RING)]
    for to in greeted:
        pl.semaphore_signal(barrier, inc=1, device_id=to, device_id_type=MESH)
    pl.semaphore_wait(barrier, len(greeted))

    base = pl.multiple_of(core * half, half)
    my_half = pl.ds(base, half)
    loads = []
    for t in range(per_piece):
        copy = pltpu.make_async_copy(
            x_ref.at[:, pl.ds(t * TILE, TILE)], own.at[t, my_half], load_sem.at[t]
        )
        copy.start()
        loads.append(copy)
    for copy in loads:
        copy.wait()
    to_sibling = remote(own.at[:, my_half], own.at[:, my_half], sib_send, sib_recv, sibling)
    to_sibling.start()
    to_near = []
    for q in range(chunks):
        rows = pl.ds(pl.multiple_of(base + q * step, step), step)
        copy = remote(
            own.at[:, rows], near.at[:, rows], near_send.at[q], near_recv.at[q], near_chip
        )
        copy.start()
        to_near.append(copy)
    first = pl.multiple_of(h * held, held)
    load_tiles = pltpu.make_async_copy(tiles_ref.at[pl.ds(first, held)], weights, tiles_sem)
    load_tiles.start()
    to_sibling.wait_recv()

    def ring_out(block, slot, which):
        copies = []
        for k in (2, 1, 3):
            p = (r + k) % RING
            rows = pl.ds(pl.multiple_of(p * quarter, quarter), quarter)
            copy = remote(
                block.at[:, rows], gathered.at[slot], ring_send.at[which, k - 1], ring_recv.at[which, k - 1], ring_peer(p)
            )
            copy.start()
            copies.append(copy)
        rows = pl.ds(pl.multiple_of(r * quarter, quarter), quarter)
        gathered[slot] = block[:, rows]
        return copies

    own_slot = pl.ds((h * RING + r) * per_piece, per_piece)
    near_slot = pl.ds(((1 - h) * RING + r) * per_piece, per_piece)

    def ring_copies(block, slot, which):
        for k in range(1, RING):
            p = (r + k) % RING
            rows = pl.ds(pl.multiple_of(p * quarter, quarter), quarter)
            remote(
                block.at[:, rows], gathered.at[slot], ring_send.at[which, k - 1], ring_recv.at[which, k - 1], ring_peer(p)
            ).wait()

    @pl.when(core == 0)
    def _():
        ring_out(own, own_slot, 0)

    @pl.when(core == 1)
    def _():
        turn(own, turned, side)
        ring_out(turned, own_slot, 0)

    def chunk_rows(of, q):
        return pl.ds(of * half + q * step, step)

    def forward(q):
        rows = pl.ds(pl.multiple_of(base + q * step, step), step)
        return remote(near.at[:, rows], far.at[:, rows], far_send.at[q], far_recv.at[q], far_chip)

    def share_near(q):
        rows = chunk_rows(0, q)
        return remote(near.at[:, rows], near.at[:, rows], share_send.at[q], share_recv.at[q], sibling)

    def share_far(q):
        rows = chunk_rows(1, q)
        return remote(far.at[:, rows], far.at[:, rows], share_send.at[q], share_recv.at[q], sibling)

    for q in range(chunks):
        to_near[q].wait_recv()
        forward(q).start()

        @pl.when(core == 0)
        def _():
            share_near(q).start()

    @pl.when(core == 0)
    def _():
        for q in range(chunks):
            forward(q).wait_recv()
        for q in range(chunks):
            share_far(q).wait_recv()
        ring_out(far, near_slot, 1)

    @pl.when(core == 1)
    def _():
        for q in range(chunks):
            share_near(q).wait_recv()
        turn(near, turned_near, side)
        ring_out(turned_near, near_slot, 1)
        for q in range(chunks):
            forward(q).wait_recv()
            share_far(q).start()

    load_tiles.wait()
    ring_copies(own, own_slot, 0)
    ring_copies(far, near_slot, 1)

    def hop_piece(p, target):
        def one_tile(t, carry):
            i = p * per_piece + t
            picked = []
            values = []
            for k in range(tile_k):
                at = (h * held + i) * tile_k + k
                picked.append(gathered[columns_ref[at]])
                sign = (1 - 2 * signs_ref[at]).astype(jnp.float32)
                values.append((weights[i, k].astype(jnp.float32) * sign).astype(jnp.bfloat16))
            left = jnp.concatenate(picked, axis=1)
            right = jnp.concatenate(values, axis=1)
            hopped = lax.dot_general(
                left, right, (((1,), (1,)), ((), ())), preferred_element_type=jnp.float32
            )
            target[t] = hopped.astype(jnp.bfloat16)
            return carry

        lax.fori_loop(0, per_piece, one_tile, 0)

    my_rows = pl.ds(pl.multiple_of(r * quarter, quarter), quarter)
    backs = []
    for k in (2, 1, 3):
        p = (r + k) % RING
        hop_piece(p, result.at[k - 1])
        copy = remote(
            result.at[k - 1], returned.at[:, my_rows], back_send.at[k - 1], back_recv.at[k - 1], ring_peer(p)
        )
        copy.start()
        backs.append(copy)
    hop_piece(r, returned.at[:, my_rows])
    for copy in backs:
        copy.wait()

    def hand_out(block, keep, give):
        copies = []
        for t in range(per_piece):
            columns = pl.ds(t * TILE, TILE)
            copy = remote(
                block.at[t, pl.ds(give, half)], other_ref.at[:, columns], last_send.at[t], last_recv.at[t], sibling
            )
            copy.start()
            copies.append(copy)
            copy = pltpu.make_async_copy(
                block.at[t, pl.ds(keep, half)], mine_ref.at[:, columns], load_sem.at[t]
            )
            copy.start()
            copies.append(copy)
        for copy in copies:
            copy.wait()

    @pl.when(core == 0)
    def _():
        hand_out(returned, 0, half)

    @pl.when(core == 1)
    def _():
        turn(returned, turned, side)
        hand_out(turned, half, 0)

    to_sibling.wait_send()
    for q in range(chunks):
        to_near[q].wait_send()
        forward(q).wait_send()

    @pl.when(core == 0)
    def _():
        for q in range(chunks):
            share_near(q).wait_send()

    @pl.when(core == 1)
    def _():
        for q in range(chunks):
            share_far(q).wait_send()


def hop_both(x, hop_tiles, columns, signs):
    half, side = x.shape
    tile_k = hop_tiles.shape[1]
    held = RING * (side // TILE)
    quarter = side // RING
    chunks = 4
    anywhere = pl.BlockSpec(memory_space=pl.ANY)
    scalars = pl.BlockSpec(memory_space=pltpu.SMEM)
    per_piece = side // TILE
    block = pltpu.VMEM((per_piece, side, TILE), jnp.bfloat16)
    dma = pltpu.SemaphoreType.DMA
    return pl.pallas_call(
        functools.partial(exchange_kernel, tile_k),
        in_specs=[scalars, scalars, anywhere, anywhere],
        out_specs=[anywhere, anywhere],
        out_shape=[jax.ShapeDtypeStruct(x.shape, jnp.bfloat16)] * 2,
        scratch_shapes=[
            block,
            block,
            block,
            block,
            block,
            pltpu.VMEM((2 * held, quarter, TILE), jnp.bfloat16),
            pltpu.VMEM((RING - 1, per_piece, quarter, TILE), jnp.bfloat16),
            block,
            pltpu.VMEM((held, tile_k, TILE, TILE), jnp.bfloat16),
            dma((per_piece,)),
            dma,
            dma,
            dma,
            dma((chunks,)),
            dma((chunks,)),
            dma((chunks,)),
            dma((chunks,)),
            dma((chunks,)),
            dma((chunks,)),
            dma((2, RING - 1)),
            dma((2, RING - 1)),
            dma((RING - 1,)),
            dma((RING - 1,)),
            dma((per_piece,)),
            dma((per_piece,)),
        ],
        compiler_params=pltpu.CompilerParams(
            collective_id=0, has_side_effects=True, vmem_limit_bytes=67043328
        ),
        cost_estimate=pl.CostEstimate(
            flops=2 * quarter * held * tile_k * TILE * TILE,
            bytes_accessed=8 * half * side + 2 * held * tile_k * TILE * TILE,
            transcendentals=0,
        ),
        name="hop_both",
    )(columns, signs, x, hop_tiles)


def sum_kernel(ups, downs, x_ref, out_ref, first, second, send_a, recv_a, send_b, recv_b):
    u = lax.axis_index("up")
    d = lax.axis_index("dn")
    barrier = pltpu.get_barrier_semaphore()
    for j in range(1, downs):
        pl.semaphore_signal(barrier, inc=1, device_id=(u, (d + j) % downs), device_id_type=MESH)
    for j in range(1, ups):
        pl.semaphore_signal(barrier, inc=1, device_id=((u + j) % ups, d), device_id_type=MESH)
    first[d] = x_ref[...]
    pl.semaphore_wait(barrier, ups + downs - 2)
    copies = []
    for j in range(1, downs):
        copy = pltpu.make_async_remote_copy(
            src_ref=x_ref, dst_ref=first.at[d], send_sem=send_a.at[j], recv_sem=recv_a.at[j],
            device_id=(u, (d + j) % downs), device_id_type=MESH,
        )
        copy.start()
        copies.append(copy)
    for copy in copies:
        copy.wait()
    total = first[0]
    for j in range(1, downs):
        total = total + first[j]
    second[u] = total
    copies = []
    for j in range(1, ups):
        copy = pltpu.make_async_remote_copy(
            src_ref=second.at[u], dst_ref=second.at[u], send_sem=send_b.at[j], recv_sem=recv_b.at[j],
            device_id=((u + j) % ups, d), device_id_type=MESH,
        )
        copy.start()
        copies.append(copy)
    for copy in copies:
        copy.wait()
    total = second[0]
    for j in range(1, ups):
        total = total + second[j]
    out_ref[...] = total


def sum_all(values):
    ups = lax.axis_size("up")
    downs = lax.axis_size("dn")
    tile = (8, TILE)
    packed = jnp.zeros(tile, jnp.float32)
    for row, value in enumerate(values):
        packed = packed.at[row].set(value)
    vmem = pl.BlockSpec(memory_space=pltpu.VMEM)
    summed = pl.pallas_call(
        functools.partial(sum_kernel, ups, downs),
        in_specs=[vmem],
        out_specs=vmem,
        out_shape=jax.ShapeDtypeStruct(tile, jnp.float32),
        scratch_shapes=[
            pltpu.VMEM((downs,) + tile, jnp.float32),
            pltpu.VMEM((ups,) + tile, jnp.float32),
            pltpu.SemaphoreType.DMA((downs,)),
            pltpu.SemaphoreType.DMA((downs,)),
            pltpu.SemaphoreType.DMA((ups,)),
            pltpu.SemaphoreType.DMA((ups,)),
        ],
        compiler_params=pltpu.CompilerParams(collective_id=1, has_side_effects=True),
        name="sum_all",
    )(packed)
    return [summed[row, 0] for row in range(len(values))]


def body(start_vector, hop_tiles, tile_columns, tile_signs, occupation):
    block_rows, block_cols = start_vector.shape
    columns = tile_columns.reshape(-1)
    signs = tile_signs.reshape(-1)
    row_start = lax.axis_index("up") * block_rows
    col_start = lax.axis_index("dn") * block_cols
    occ_rows = lax.dynamic_slice_in_dim(occupation, row_start, block_rows, 1).astype(jnp.bfloat16)
    occ_cols = lax.dynamic_slice_in_dim(occupation, col_start, block_cols, 1).astype(jnp.bfloat16)
    diagonal = (
        coupling * jnp.einsum("sa,sb->ab", occ_rows, occ_cols, preferred_element_type=jnp.float32)
    ).astype(jnp.bfloat16)
    start = start_vector.astype(jnp.float32)
    mine, other = hop_both(start_vector, hop_tiles, columns, signs)
    work = mine.astype(jnp.float32) + other.astype(jnp.float32) + diagonal * start
    total, cross, square = sum_all(
        [jnp.sum(start * start), jnp.sum(work * start), jnp.sum(work * work)]
    )
    scale = 1.0 / jnp.maximum(jnp.sqrt(total), 1.0)
    length = total / jnp.maximum(total, 1.0)
    alpha = cross * scale * scale
    residual = square * scale * scale - 2.0 * alpha * alpha + alpha * alpha * length
    beta = jnp.sqrt(jnp.maximum(residual, 1.0))
    alphas, betas = [alpha], [beta]
    length = residual / jnp.maximum(residual, 1.0)
    previous = start * scale
    vector = (work * scale - alpha * previous) / beta
    for _ in range(STEPS - 1):
        mine, other = hop_both(vector.astype(jnp.bfloat16), hop_tiles, columns, signs)
        work = mine.astype(jnp.float32) + other.astype(jnp.float32) + diagonal * vector - beta * previous
        alpha, square = sum_all([jnp.sum(work * vector), jnp.sum(work * work)])
        residual = square - 2.0 * alpha * alpha + alpha * alpha * length
        beta = jnp.sqrt(jnp.maximum(residual, 1.0))
        alphas.append(alpha)
        betas.append(beta)
        length = residual / jnp.maximum(residual, 1.0)
        previous, vector = vector, (work - alpha * vector) / beta
    return (vector.astype(jnp.bfloat16), jnp.stack(alphas), jnp.stack(betas))


def solution(mesh):
    placed = (P("up", "dn"), P(), P(), P(), P())
    return jax.shard_map(
        body, mesh=mesh, in_specs=placed, out_specs=(P("up", "dn"), P(), P()), check_vma=False
    )
```

```python
import functools

import jax
import jax.numpy as jnp
from jax import lax
from jax.experimental import pallas as pl
from jax.experimental.pallas import tpu as pltpu
from jax.sharding import PartitionSpec as P

STEPS = 2
RING = 4
TILE = 128
MESH = pl.DeviceIdType.MESH

coupling = 4.0


def place():
    u = lax.axis_index("up")
    d = lax.axis_index("dn")
    return u // 8, (u // 2) % 4, u % 2, d // 4, d % 4


def device(y_lo, x, core, y_hi, z):
    return (y_lo * 8 + x * 2 + core, y_hi * 4 + z)


def turn_tile(source, target, i, tiles):
    for j in range(tiles):
        target[i, j * TILE : (j + 1) * TILE, :] = source[j, i * TILE : (i + 1) * TILE, :].T


PARTS = 2
CUTS = (112, 96)
CHUNKS = 8
GROUPS = {1: ((0, 1), (7, 1)), 3: ((1, 2), (8, 1)), 5: ((3, 1), (9, 2)), 7: ((4, 3), (11, 2))}
GROUP_AT = {0: 0, 7: 1, 1: 2, 8: 3, 3: 4, 9: 5, 4: 6, 11: 7}


def exchange_kernel(
    tile_k,
    columns_ref,
    signs_ref,
    x_ref,
    tiles_ref,
    mine_ref,
    other_ref,
    own,
    near,
    far,
    turned,
    turned_near,
    gathered_a,
    gathered_b,
    result,
    returned,
    weights,
    load_sem,
    tiles_sem,
    sib_send,
    sib_recv,
    near_send,
    near_recv,
    far_send,
    far_recv,
    share_send,
    share_recv,
    ring_send,
    ring_recv,
    late_send,
    late_recv,
    back_send,
    back_recv,
    last_send,
    last_recv,
):
    half = x_ref.shape[0]
    side = 2 * half
    quarter = side // RING
    piece = quarter // PARTS
    per_piece = side // TILE
    held = RING * per_piece
    gathered = (gathered_a, gathered_b)
    y_lo, x, core, y_hi, z = place()
    r = z + core * (x - z)
    h = y_hi + core * (y_lo - y_hi)
    sibling = device(y_lo, x, 1 - core, y_hi, z)
    near_chip = device(1 - y_lo, x, core, y_hi, z)
    far_chip = device(1 - y_lo, x, core, 1 - y_hi, z)

    def ring_peer(p):
        return device(y_lo, x + core * (p - x), core, y_hi, p + core * (z - p))

    def remote(src, dst, send, recv, to):
        return pltpu.make_async_remote_copy(
            src_ref=src, dst_ref=dst, send_sem=send, recv_sem=recv, device_id=to, device_id_type=MESH
        )

    def rows_of(p, part):
        start = (p // 2) * half + (p % 2) * piece + part * quarter
        return pl.ds(pl.multiple_of(start, 16), piece)

    starts = [(q // 2) * piece + (q % 2) * CUTS[0] for q in range(CHUNKS)]
    sizes = [CUTS[q % 2] for q in range(CHUNKS)]

    barrier = pltpu.get_barrier_semaphore()
    greeted = [sibling, near_chip, far_chip] + [ring_peer((r + k) % RING) for k in range(1, RING)]
    for to in greeted:
        pl.semaphore_signal(barrier, inc=1, device_id=to, device_id_type=MESH)

    base = pl.multiple_of(core * half, half)
    my_half = pl.ds(base, half)
    loads = []
    for t in range(per_piece):
        copy = pltpu.make_async_copy(
            x_ref.at[:, pl.ds(t * TILE, TILE)], own.at[t, my_half], load_sem.at[t]
        )
        copy.start()
        loads.append(copy)
    with jax.named_scope("barrier"):
        pl.semaphore_wait(barrier, len(greeted))
    with jax.named_scope("load"):
        for copy in loads:
            copy.wait()
    to_sibling = remote(own.at[:, my_half], own.at[:, my_half], sib_send, sib_recv, sibling)
    to_sibling.start()

    def to_near(q):
        rows = pl.ds(pl.multiple_of(base + starts[q], 16), sizes[q])
        return remote(own.at[:, rows], near.at[:, rows], near_send.at[q], near_recv.at[q], near_chip)

    for q in range(CHUNKS):
        to_near(q).start()
    first = pl.multiple_of(h * held, held)
    load_tiles = pltpu.make_async_copy(tiles_ref.at[pl.ds(first, held)], weights, tiles_sem)
    load_tiles.start()
    with jax.named_scope("sibling"):
        to_sibling.wait_recv()

    own_slot = pl.ds((h * RING + r) * per_piece, per_piece)
    near_start = ((1 - h) * RING + r) * per_piece
    near_slot = pl.ds(near_start, per_piece)

    def own_copy(block, part, k):
        p = (r + k) % RING
        return remote(
            block.at[:, rows_of(p, part)],
            gathered[part].at[own_slot],
            ring_send.at[part, k - 1],
            ring_recv.at[part, k - 1],
            ring_peer(p),
        )

    def own_out(block):
        for part in range(PARTS):
            for k in (2, 1, 3):
                own_copy(block, part, k).start()
        for part in range(PARTS):
            gathered[part][own_slot] = block[:, rows_of(r, part)]

    @pl.when(core == 0)
    def _():
        own_out(own)

    @pl.when(core == 1)
    def _():
        with jax.named_scope("turn_own"):
            for i in range(per_piece):
                turn_tile(own, turned, i, per_piece)
        own_out(turned)

    def half_rows(of, q):
        return pl.ds(of * half + starts[q], sizes[q])

    def forward(q):
        rows = pl.ds(pl.multiple_of(base + starts[q], 16), sizes[q])
        return remote(near.at[:, rows], far.at[:, rows], far_send.at[q], far_recv.at[q], far_chip)

    def share_near(q):
        rows = half_rows(0, q)
        return remote(near.at[:, rows], near.at[:, rows], share_send.at[q], share_recv.at[q], sibling)

    def share_far(q):
        rows = half_rows(1, q)
        return remote(far.at[:, rows], far.at[:, rows], share_send.at[q], share_recv.at[q], sibling)

    def late_down(of, q):
        p = 2 * of + (q // 2) % 2
        part, sub = q // 4, q % 2
        k = (p - r) % RING
        at = (part * 2 + sub) * RING + k
        rows = pl.ds(sub * CUTS[0], sizes[q])
        return p, remote(
            far.at[:, half_rows(of, q)],
            gathered[part].at[near_slot, rows],
            late_send.at[at],
            late_recv.at[at],
            ring_peer(p),
        )

    def pass_down(of, q):
        p, copy = late_down(of, q)

        @pl.when(p != r)
        def _():
            copy.start()

        @pl.when(p == r)
        def _():
            part, sub = q // 4, q % 2
            gathered[part][near_slot, sub * CUTS[0] : sub * CUTS[0] + sizes[q]] = far[:, half_rows(of, q)]

    def late_up(start, count, part, k):
        p = (r + k) % RING
        at = (GROUP_AT[start] * PARTS + part) * RING + k
        tiles = pl.ds(start, count)
        return remote(
            turned_near.at[tiles, rows_of(p, part)],
            gathered[part].at[pl.ds(near_start + start, count)],
            late_send.at[at],
            late_recv.at[at],
            ring_peer(p),
        )

    def pass_up(start, count):
        for i in range(start, start + count):
            turn_tile(near, turned_near, i, per_piece)
        for part in range(PARTS):
            for k in (2, 1, 3):
                late_up(start, count, part, k).start()
        tiles = pl.ds(start, count)
        for part in range(PARTS):
            gathered[part][pl.ds(near_start + start, count)] = turned_near[tiles, rows_of(r, part)]

    @pl.when(core == 0)
    def _():
        for q in range(CHUNKS + 1):
            if q < CHUNKS:
                with jax.named_scope(f"near{q}"):
                    to_near(q).wait_recv()
                forward(q).start()
                share_near(q).start()
            if q >= 1:
                with jax.named_scope(f"far{q - 1}"):
                    forward(q - 1).wait_recv()
                pass_down(0, q - 1)
                with jax.named_scope(f"share{q - 1}"):
                    share_far(q - 1).wait_recv()
                pass_down(1, q - 1)

    @pl.when(core == 1)
    def _():
        for q in range(CHUNKS + 1):
            if q < CHUNKS:
                with jax.named_scope(f"near{q}"):
                    to_near(q).wait_recv()
                forward(q).start()
            if q >= 1:
                with jax.named_scope(f"far{q - 1}"):
                    forward(q - 1).wait_recv()
                share_far(q - 1).start()
            if q < CHUNKS:
                with jax.named_scope(f"share{q}"):
                    share_near(q).wait_recv()
                for start, count in GROUPS.get(q, ()):
                    pass_up(start, count)

    with jax.named_scope("tiles"):
        load_tiles.wait()

    def arrivals(part):
        for k in range(1, RING):
            own_copy(own, part, k).wait_recv()

        @pl.when(core == 0)
        def _():
            for sub in range(2):
                for k in range(1, RING):
                    at = (part * 2 + sub) * RING + k
                    rows = pl.ds(sub * CUTS[0], CUTS[sub])
                    remote(
                        far.at[:, rows],
                        gathered[part].at[near_slot, rows],
                        late_send.at[at],
                        late_recv.at[at],
                        ring_peer((r + k) % RING),
                    ).wait_recv()

        @pl.when(core == 1)
        def _():
            for groups in GROUPS.values():
                for start, count in groups:
                    for k in range(1, RING):
                        late_up(start, count, part, k).wait_recv()

    def hop_piece(part, p, target):
        def one_tile(t, carry):
            i = p * per_piece + t
            picked = []
            values = []
            for k in range(tile_k):
                at = (h * held + i) * tile_k + k
                picked.append(gathered[part][columns_ref[at]])
                sign = (1 - 2 * signs_ref[at]).astype(jnp.float32)
                values.append((weights[i, k].astype(jnp.float32) * sign).astype(jnp.bfloat16))
            left = jnp.concatenate(picked, axis=1)
            right = jnp.concatenate(values, axis=1)
            hopped = lax.dot_general(
                left, right, (((1,), (1,)), ((), ())), preferred_element_type=jnp.float32
            )
            target[t] = hopped.astype(jnp.bfloat16)
            return carry

        lax.fori_loop(0, per_piece, one_tile, 0)

    def back_copy(part, k):
        return remote(
            result.at[part, k - 1],
            returned.at[:, rows_of(r, part)],
            back_send.at[part, k - 1],
            back_recv.at[part, k - 1],
            ring_peer((r + k) % RING),
        )

    for part in range(PARTS):
        with jax.named_scope(f"arrive{part}"):
            arrivals(part)
        with jax.named_scope(f"hop{part}"):
            for k in (2, 1, 3):
                hop_piece(part, (r + k) % RING, result.at[part, k - 1])
                back_copy(part, k).start()
            hop_piece(part, r, returned.at[:, rows_of(r, part)])
    with jax.named_scope("back"):
        for part in range(PARTS):
            for k in range(1, RING):
                back_copy(part, k).wait()

    def hand_out(block, keep, give):
        copies = []
        for t in range(per_piece):
            columns = pl.ds(t * TILE, TILE)
            copy = remote(
                block.at[t, pl.ds(give, half)], other_ref.at[:, columns], last_send.at[t], last_recv.at[t], sibling
            )
            copy.start()
            copies.append(copy)
            copy = pltpu.make_async_copy(
                block.at[t, pl.ds(keep, half)], mine_ref.at[:, columns], load_sem.at[t]
            )
            copy.start()
            copies.append(copy)
        for copy in copies:
            copy.wait()

    for part in range(PARTS):
        for k in range(1, RING):
            own_copy(own, part, k).wait_send()

    @pl.when(core == 0)
    def _():
        with jax.named_scope("out0"):
            hand_out(returned, 0, half)

    @pl.when(core == 1)
    def _():
        with jax.named_scope("turn_back"):
            for i in range(per_piece):
                turn_tile(returned, turned, i, per_piece)
        with jax.named_scope("out1"):
            hand_out(turned, half, 0)

    to_sibling.wait_send()
    for q in range(CHUNKS):
        to_near(q).wait_send()
        forward(q).wait_send()

    @pl.when(core == 0)
    def _():
        for q in range(CHUNKS):
            share_near(q).wait_send()
            for of in range(2):
                p, copy = late_down(of, q)

                @pl.when(p != r)
                def _():
                    copy.wait_send()

    @pl.when(core == 1)
    def _():
        for q in range(CHUNKS):
            share_far(q).wait_send()
        for groups in GROUPS.values():
            for start, count in groups:
                for part in range(PARTS):
                    for k in range(1, RING):
                        late_up(start, count, part, k).wait_send()


def hop_both(x, hop_tiles, columns, signs):
    half, side = x.shape
    tile_k = hop_tiles.shape[1]
    held = RING * (side // TILE)
    quarter = side // RING
    piece = quarter // PARTS
    anywhere = pl.BlockSpec(memory_space=pl.ANY)
    scalars = pl.BlockSpec(memory_space=pltpu.SMEM)
    per_piece = side // TILE
    block = pltpu.VMEM((per_piece, side, TILE), jnp.bfloat16)
    dma = pltpu.SemaphoreType.DMA
    return pl.pallas_call(
        functools.partial(exchange_kernel, tile_k),
        in_specs=[scalars, scalars, anywhere, anywhere],
        out_specs=[anywhere, anywhere],
        out_shape=[jax.ShapeDtypeStruct(x.shape, jnp.bfloat16)] * 2,
        scratch_shapes=[
            block,
            block,
            block,
            block,
            block,
            pltpu.VMEM((2 * held, piece, TILE), jnp.bfloat16),
            pltpu.VMEM((2 * held, piece, TILE), jnp.bfloat16),
            pltpu.VMEM((PARTS, RING - 1, per_piece, piece, TILE), jnp.bfloat16),
            block,
            pltpu.VMEM((held, tile_k, TILE, TILE), jnp.bfloat16),
            dma((per_piece,)),
            dma,
            dma,
            dma,
            dma((CHUNKS,)),
            dma((CHUNKS,)),
            dma((CHUNKS,)),
            dma((CHUNKS,)),
            dma((CHUNKS,)),
            dma((CHUNKS,)),
            dma((PARTS, RING - 1)),
            dma((PARTS, RING - 1)),
            dma((len(GROUP_AT) * PARTS * RING,)),
            dma((len(GROUP_AT) * PARTS * RING,)),
            dma((PARTS, RING - 1)),
            dma((PARTS, RING - 1)),
            dma((per_piece,)),
            dma((per_piece,)),
        ],
        compiler_params=pltpu.CompilerParams(
            collective_id=0, has_side_effects=True, vmem_limit_bytes=67043328
        ),
        cost_estimate=pl.CostEstimate(
            flops=2 * quarter * held * tile_k * TILE * TILE,
            bytes_accessed=8 * half * side + 2 * held * tile_k * TILE * TILE,
            transcendentals=0,
        ),
        name="hop_both",
    )(columns, signs, x, hop_tiles)


def sum_kernel(ups, downs, x_ref, out_ref, first, second, send_a, recv_a, send_b, recv_b):
    u = lax.axis_index("up")
    d = lax.axis_index("dn")
    barrier = pltpu.get_barrier_semaphore()
    for j in range(1, downs):
        pl.semaphore_signal(barrier, inc=1, device_id=(u, (d + j) % downs), device_id_type=MESH)
    for j in range(1, ups):
        pl.semaphore_signal(barrier, inc=1, device_id=((u + j) % ups, d), device_id_type=MESH)
    first[d] = x_ref[...]
    pl.semaphore_wait(barrier, ups + downs - 2)
    copies = []
    for j in range(1, downs):
        copy = pltpu.make_async_remote_copy(
            src_ref=x_ref, dst_ref=first.at[d], send_sem=send_a.at[j], recv_sem=recv_a.at[j],
            device_id=(u, (d + j) % downs), device_id_type=MESH,
        )
        copy.start()
        copies.append(copy)
    for copy in copies:
        copy.wait()
    total = first[0]
    for j in range(1, downs):
        total = total + first[j]
    second[u] = total
    copies = []
    for j in range(1, ups):
        copy = pltpu.make_async_remote_copy(
            src_ref=second.at[u], dst_ref=second.at[u], send_sem=send_b.at[j], recv_sem=recv_b.at[j],
            device_id=((u + j) % ups, d), device_id_type=MESH,
        )
        copy.start()
        copies.append(copy)
    for copy in copies:
        copy.wait()
    total = second[0]
    for j in range(1, ups):
        total = total + second[j]
    out_ref[...] = total


def sum_all(values):
    ups = lax.axis_size("up")
    downs = lax.axis_size("dn")
    tile = (8, TILE)
    packed = jnp.zeros(tile, jnp.float32)
    for row, value in enumerate(values):
        packed = packed.at[row].set(value)
    vmem = pl.BlockSpec(memory_space=pltpu.VMEM)
    summed = pl.pallas_call(
        functools.partial(sum_kernel, ups, downs),
        in_specs=[vmem],
        out_specs=vmem,
        out_shape=jax.ShapeDtypeStruct(tile, jnp.float32),
        scratch_shapes=[
            pltpu.VMEM((downs,) + tile, jnp.float32),
            pltpu.VMEM((ups,) + tile, jnp.float32),
            pltpu.SemaphoreType.DMA((downs,)),
            pltpu.SemaphoreType.DMA((downs,)),
            pltpu.SemaphoreType.DMA((ups,)),
            pltpu.SemaphoreType.DMA((ups,)),
        ],
        compiler_params=pltpu.CompilerParams(collective_id=1, has_side_effects=True),
        name="sum_all",
    )(packed)
    return [summed[row, 0] for row in range(len(values))]


def body(start_vector, hop_tiles, tile_columns, tile_signs, occupation):
    block_rows, block_cols = start_vector.shape
    columns = tile_columns.reshape(-1)
    signs = tile_signs.reshape(-1)
    row_start = lax.axis_index("up") * block_rows
    col_start = lax.axis_index("dn") * block_cols
    occ_rows = lax.dynamic_slice_in_dim(occupation, row_start, block_rows, 1).astype(jnp.bfloat16)
    occ_cols = lax.dynamic_slice_in_dim(occupation, col_start, block_cols, 1).astype(jnp.bfloat16)
    diagonal = (
        coupling * jnp.einsum("sa,sb->ab", occ_rows, occ_cols, preferred_element_type=jnp.float32)
    ).astype(jnp.bfloat16)
    start = start_vector.astype(jnp.float32)
    mine, other = hop_both(start_vector, hop_tiles, columns, signs)
    work = mine.astype(jnp.float32) + other.astype(jnp.float32) + diagonal * start
    total, cross, square = sum_all(
        [jnp.sum(start * start), jnp.sum(work * start), jnp.sum(work * work)]
    )
    scale = 1.0 / jnp.maximum(jnp.sqrt(total), 1.0)
    length = total / jnp.maximum(total, 1.0)
    alpha = cross * scale * scale
    residual = square * scale * scale - 2.0 * alpha * alpha + alpha * alpha * length
    beta = jnp.sqrt(jnp.maximum(residual, 1.0))
    alphas, betas = [alpha], [beta]
    length = residual / jnp.maximum(residual, 1.0)
    previous = start * scale
    vector = (work * scale - alpha * previous) / beta
    for _ in range(STEPS - 1):
        mine, other = hop_both(vector.astype(jnp.bfloat16), hop_tiles, columns, signs)
        work = mine.astype(jnp.float32) + other.astype(jnp.float32) + diagonal * vector - beta * previous
        alpha, square = sum_all([jnp.sum(work * vector), jnp.sum(work * work)])
        residual = square - 2.0 * alpha * alpha + alpha * alpha * length
        beta = jnp.sqrt(jnp.maximum(residual, 1.0))
        alphas.append(alpha)
        betas.append(beta)
        length = residual / jnp.maximum(residual, 1.0)
        previous, vector = vector, (work - alpha * vector) / beta
    return (vector.astype(jnp.bfloat16), jnp.stack(alphas), jnp.stack(betas))


def solution(mesh):
    placed = (P("up", "dn"), P(), P(), P(), P())
    return jax.shard_map(
        body, mesh=mesh, in_specs=placed, out_specs=(P("up", "dn"), P(), P()), check_vma=False
    )
```

```python
import functools

import jax
import jax.numpy as jnp
from jax import lax
from jax.experimental import pallas as pl
from jax.experimental.pallas import tpu as pltpu
from jax.sharding import PartitionSpec as P

STEPS = 2
RING = 4
TILE = 128
MESH = pl.DeviceIdType.MESH

coupling = 4.0


def place():
    u = lax.axis_index("up")
    d = lax.axis_index("dn")
    return u // 8, (u // 2) % 4, u % 2, d // 4, d % 4


def device(y_lo, x, core, y_hi, z):
    return (y_lo * 8 + x * 2 + core, y_hi * 4 + z)


def turn_tile(source, target, i, tiles):
    for j in range(tiles):
        target[i, j * TILE : (j + 1) * TILE, :] = source[j, i * TILE : (i + 1) * TILE, :].T


PARTS = 2
CUTS = (112, 96)
CHUNKS = 8
GROUPS = {
    1: ((0, 1), (7, 1)),
    3: ((1, 2), (8, 1)),
    5: ((3, 1), (9, 2)),
    6: ((4, 1), (11, 1)),
    7: ((5, 2), (12, 1)),
}
GROUP_AT = {start: at for at, start in enumerate(g[0] for gs in GROUPS.values() for g in gs)}
ROWS = 8


def recurrence_kernel(
    tile_k,
    columns_ref,
    signs_ref,
    x_ref,
    tiles_ref,
    occ_rows,
    occ_cols,
    shift_ref,
    out_ref,
    numbers_ref,
    own,
    near,
    far,
    turned,
    turned_near,
    gathered_a,
    gathered_b,
    result,
    returned,
    weights,
    kept,
    hopped_kept,
    sums,
    first,
    second,
    factors,
    load_sem,
    tiles_sem,
    sib_send,
    sib_recv,
    near_send,
    near_recv,
    far_send,
    far_recv,
    share_send,
    share_recv,
    ring_send,
    ring_recv,
    late_send,
    late_recv,
    back_send,
    back_recv,
    swap_send,
    swap_recv,
    down_send,
    down_recv,
    up_send,
    up_recv,
    free_sem,
    ready_sem,
):
    half = x_ref.shape[0]
    side = 2 * half
    quarter = side // RING
    piece = quarter // PARTS
    per_piece = side // TILE
    held = RING * per_piece
    gathered = (gathered_a, gathered_b)
    y_lo, x, core, y_hi, z = place()
    u = lax.axis_index("up")
    d = lax.axis_index("dn")
    ups = lax.axis_size("up")
    downs = lax.axis_size("dn")
    r = z + core * (x - z)
    h = y_hi + core * (y_lo - y_hi)
    sibling = device(y_lo, x, 1 - core, y_hi, z)
    near_chip = device(1 - y_lo, x, core, y_hi, z)
    far_chip = device(1 - y_lo, x, core, 1 - y_hi, z)

    def ring_peer(p):
        return device(y_lo, x + core * (p - x), core, y_hi, p + core * (z - p))

    def remote(src, dst, send, recv, to):
        return pltpu.make_async_remote_copy(
            src_ref=src, dst_ref=dst, send_sem=send, recv_sem=recv, device_id=to, device_id_type=MESH
        )

    def rows_of(p, part):
        start = (p // 2) * half + (p % 2) * piece + part * quarter
        return pl.ds(pl.multiple_of(start, 16), piece)

    starts = [(q // 2) * piece + (q % 2) * CUTS[0] for q in range(CHUNKS)]
    sizes = [CUTS[q % 2] for q in range(CHUNKS)]

    barrier = pltpu.get_barrier_semaphore()
    greeted = [sibling, near_chip, far_chip] + [ring_peer((r + k) % RING) for k in range(1, RING)]
    for to in greeted:
        pl.semaphore_signal(barrier, inc=1, device_id=to, device_id_type=MESH)
    for j in range(1, downs):
        pl.semaphore_signal(barrier, inc=1, device_id=(u, (d + j) % downs), device_id_type=MESH)
    for j in range(1, ups):
        pl.semaphore_signal(barrier, inc=1, device_id=((u + j) % ups, d), device_id_type=MESH)

    base = pl.multiple_of(core * half, half)
    my_half = pl.ds(base, half)
    loads = []
    for t in range(per_piece):
        copy = pltpu.make_async_copy(
            x_ref.at[:, pl.ds(t * TILE, TILE)], own.at[t, my_half], load_sem.at[t]
        )
        copy.start()
        loads.append(copy)
    first_tile = pl.multiple_of(h * held, held)
    load_tiles = pltpu.make_async_copy(tiles_ref.at[pl.ds(first_tile, held)], weights, tiles_sem)
    load_tiles.start()
    with jax.named_scope("barrier"):
        pl.semaphore_wait(barrier, len(greeted) + downs + ups - 2)
    with jax.named_scope("load"):
        for copy in loads:
            copy.wait()
        load_tiles.wait()

    own_slot = pl.ds((h * RING + r) * per_piece, per_piece)
    near_start = ((1 - h) * RING + r) * per_piece
    near_slot = pl.ds(near_start, per_piece)

    to_sibling = remote(own.at[:, my_half], own.at[:, my_half], sib_send, sib_recv, sibling)

    def to_near(q):
        rows = pl.ds(pl.multiple_of(base + starts[q], 16), sizes[q])
        return remote(own.at[:, rows], near.at[:, rows], near_send.at[q], near_recv.at[q], near_chip)

    def own_copy(block, part, k):
        p = (r + k) % RING
        return remote(
            block.at[:, rows_of(p, part)],
            gathered[part].at[own_slot],
            ring_send.at[part, k - 1],
            ring_recv.at[part, k - 1],
            ring_peer(p),
        )

    def own_out(block):
        for part in range(PARTS):
            for k in (2, 1, 3):
                own_copy(block, part, k).start()
        for part in range(PARTS):
            gathered[part][own_slot] = block[:, rows_of(r, part)]

    def half_rows(of, q):
        return pl.ds(of * half + starts[q], sizes[q])

    def forward(q):
        rows = pl.ds(pl.multiple_of(base + starts[q], 16), sizes[q])
        return remote(near.at[:, rows], far.at[:, rows], far_send.at[q], far_recv.at[q], far_chip)

    def share_near(q):
        rows = half_rows(0, q)
        return remote(near.at[:, rows], near.at[:, rows], share_send.at[q], share_recv.at[q], sibling)

    def share_far(q):
        rows = half_rows(1, q)
        return remote(far.at[:, rows], far.at[:, rows], share_send.at[q], share_recv.at[q], sibling)

    def late_down(of, q):
        p = 2 * of + (q // 2) % 2
        part, sub = q // 4, q % 2
        at = (part * 2 + sub) * RING + (p - r) % RING
        rows = pl.ds(sub * CUTS[0], sizes[q])
        return p, remote(
            far.at[:, half_rows(of, q)],
            gathered[part].at[near_slot, rows],
            late_send.at[at],
            late_recv.at[at],
            ring_peer(p),
        )

    def pass_down(of, q):
        p, copy = late_down(of, q)

        @pl.when(p != r)
        def _():
            copy.start()

        @pl.when(p == r)
        def _():
            part, sub = q // 4, q % 2
            gathered[part][near_slot, sub * CUTS[0] : sub * CUTS[0] + sizes[q]] = far[:, half_rows(of, q)]

    def late_up(start, count, part, k):
        p = (r + k) % RING
        at = (GROUP_AT[start] * PARTS + part) * RING + k
        tiles = pl.ds(start, count)
        return remote(
            turned_near.at[tiles, rows_of(p, part)],
            gathered[part].at[pl.ds(near_start + start, count)],
            late_send.at[at],
            late_recv.at[at],
            ring_peer(p),
        )

    def pass_up(start, count):
        for i in range(start, start + count):
            turn_tile(near, turned_near, i, per_piece)
        for part in range(PARTS):
            for k in (2, 1, 3):
                late_up(start, count, part, k).start()
        tiles = pl.ds(start, count)
        for part in range(PARTS):
            gathered[part][pl.ds(near_start + start, count)] = turned_near[tiles, rows_of(r, part)]

    def arrivals_down(part):
        for k in range(1, RING):
            own_copy(own, part, k).wait_recv()
        for sub in range(2):
            for k in range(1, RING):
                at = (part * 2 + sub) * RING + k
                rows = pl.ds(sub * CUTS[0], CUTS[sub])
                remote(
                    far.at[:, rows],
                    gathered[part].at[near_slot, rows],
                    late_send.at[at],
                    late_recv.at[at],
                    ring_peer((r + k) % RING),
                ).wait_recv()

    def arrivals_up(part):
        for k in range(1, RING):
            own_copy(own, part, k).wait_recv()
        for groups in GROUPS.values():
            for start, count in groups:
                for k in range(1, RING):
                    late_up(start, count, part, k).wait_recv()

    def hop_piece(part, p, target):
        def one_tile(t, carry):
            i = p * per_piece + t
            picked = []
            values = []
            for k in range(tile_k):
                at = (h * held + i) * tile_k + k
                picked.append(gathered[part][columns_ref[at]])
                sign = (1 - 2 * signs_ref[at]).astype(jnp.float32)
                values.append((weights[i, k].astype(jnp.float32) * sign).astype(jnp.bfloat16))
            left = jnp.concatenate(picked, axis=1)
            right = jnp.concatenate(values, axis=1)
            hopped = lax.dot_general(
                left, right, (((1,), (1,)), ((), ())), preferred_element_type=jnp.float32
            )
            target[t] = hopped.astype(jnp.bfloat16)
            return carry

        lax.fori_loop(0, per_piece, one_tile, 0)

    def back_copy(part, k):
        return remote(
            result.at[part, k - 1],
            returned.at[:, rows_of(r, part)],
            back_send.at[part, k - 1],
            back_recv.at[part, k - 1],
            ring_peer((r + k) % RING),
        )

    def hop_to(part, k):
        with jax.named_scope(f"hop{part}{k}"):
            if k:
                hop_piece(part, (r + k) % RING, result.at[part, k - 1])
                back_copy(part, k).start()
            else:
                hop_piece(part, r, returned.at[:, rows_of(r, part)])

    order = (2, 1, 3, 0)

    def sum_down(use, j):
        return remote(
            first.at[use, d], first.at[use, d], down_send.at[use, j], down_recv.at[use, j], (u, (d + j) % downs)
        )

    def sum_up(use, j):
        return remote(
            second.at[use, u], second.at[use, u], up_send.at[use, j], up_recv.at[use, j], ((u + j) % ups, d)
        )

    def sum_start(use):
        first[use, d] = sums[...]
        for j in range(1, downs):
            sum_down(use, j).start()

    def sum_middle(use):
        for j in range(1, downs):
            sum_down(use, j).wait()
        total = first[use, 0]
        for j in range(1, downs):
            total = total + first[use, j]
        second[use, u] = total
        for j in range(1, ups):
            sum_up(use, j).start()

    def sum_end(use):
        for j in range(1, ups):
            sum_up(use, j).wait()
        total = second[use, 0]
        for j in range(1, ups):
            total = total + second[use, j]
        parts = [total[ROWS * i : ROWS * (i + 1)] for i in range(3)]
        return [jnp.sum(jnp.sum(part, axis=0, keepdims=True), axis=1, keepdims=True) for part in parts]

    def keep_factor(row, value):
        factors[row : row + 1, :] = jnp.broadcast_to(value, (1, TILE))

    def first_numbers():
        total, cross, square = sum_end(0)
        shift = shift_ref[0:1, 0:1]
        scale = 1.0 / jnp.maximum(jnp.sqrt(total), 1.0)
        alpha = scale * scale * (cross + shift * total)
        delta = alpha - shift
        residual = scale * scale * (square - 2.0 * delta * cross + delta * delta * total)
        beta = jnp.sqrt(jnp.maximum(residual, 1.0))
        keep_factor(0, delta)
        keep_factor(1, scale / beta)
        keep_factor(2, beta * scale)
        keep_factor(3, alpha)
        keep_factor(4, beta)

    def last_numbers():
        total, cross, square = sum_end(1)
        shift = shift_ref[0:1, 0:1]
        alpha = cross + shift * total
        delta = alpha - shift
        residual = square - 2.0 * delta * cross + delta * delta * total
        beta = jnp.sqrt(jnp.maximum(residual, 1.0))
        keep_factor(5, delta)
        keep_factor(6, 1.0 / beta)
        numbers_ref[...] = jnp.zeros_like(numbers_ref)
        numbers_ref[0:1, :] = factors[3:4, :]
        numbers_ref[1:2, :] = jnp.broadcast_to(alpha, (1, TILE))
        numbers_ref[2:3, :] = factors[4:5, :]
        numbers_ref[3:4, :] = jnp.broadcast_to(beta, (1, TILE))

    def swap(block, t, side_of):
        rows = pl.ds((1 - side_of) * half, half)
        return remote(
            block.at[t, rows], turned_near.at[t, rows], swap_send.at[t], swap_recv.at[t], sibling
        )

    def fold(value):
        return jnp.sum(value.reshape(-1, ROWS, TILE), axis=0)

    def each_block(side_of, block, act, waits):
        sums[...] = jnp.zeros_like(sums)

        def one_tile(t, carry):
            if waits:
                swap(block, t, side_of).wait_recv()
            for a in range(RING):
                rows = slice(side_of * half + a * piece, side_of * half + (a + 1) * piece)
                mine = slice(a * piece, (a + 1) * piece)
                count = jnp.dot(occ_rows[mine, :], occ_cols[t], preferred_element_type=jnp.float32)
                offset = coupling * count - shift_ref[0:1, :]
                hopped = block[t, rows].astype(jnp.float32) + turned_near[t, rows].astype(jnp.float32)
                found = act(t, rows, mine, offset, hopped)
                if found is not None:
                    for i, value in enumerate(found):
                        sums[ROWS * i : ROWS * (i + 1), :] += fold(value)
            return carry

        lax.fori_loop(0, per_piece, one_tile, 0)

    def first_work(t, rows, mine, offset, hopped):
        start = own[t, rows]
        kept[t, mine] = start
        hopped_kept[t, mine] = hopped.astype(jnp.bfloat16)
        start = start.astype(jnp.float32)
        work = hopped + offset * start
        own[t, rows] = work.astype(jnp.bfloat16)
        return start * start, work * start, work * work

    def second_work(t, rows, mine, offset, hopped):
        delta, gain, push = factors[0:1, :], factors[1:2, :], factors[2:3, :]
        start = kept[t, mine].astype(jnp.float32)
        before = own[t, rows].astype(jnp.float32) - delta * start
        vector = gain * before
        held_hop = hopped_kept[t, mine].astype(jnp.float32)
        work = gain * (hopped - delta * held_hop + offset * before) - push * start
        return vector, work

    def second_sums(t, rows, mine, offset, hopped):
        vector, work = second_work(t, rows, mine, offset, hopped)
        return vector * vector, work * vector, work * work

    def finish(t, rows, mine, offset, hopped):
        vector, work = second_work(t, rows, mine, offset, hopped)
        final = (work - factors[5:6, :] * vector) * factors[6:7, :]
        hopped_kept[t, mine] = final.astype(jnp.bfloat16)

    def one_step(step, carry):
        to_sibling.start()
        for q in range(CHUNKS):
            to_near(q).start()
        with jax.named_scope("sibling"):
            to_sibling.wait_recv()

        @pl.when(core == 0)
        def _():
            own_out(own)

        @pl.when(core == 1)
        def _():
            with jax.named_scope("turn_own"):
                for i in range(per_piece):
                    turn_tile(own, turned, i, per_piece)
            own_out(turned)

        @pl.when(step == 1)
        def _():
            sum_middle(0)

        @pl.when(core == 0)
        def _():
            for q in range(CHUNKS + 1):
                if q < CHUNKS:
                    with jax.named_scope(f"near{q}"):
                        to_near(q).wait_recv()
                    forward(q).start()
                    share_near(q).start()
                if q >= 1:
                    with jax.named_scope(f"far{q - 1}"):
                        forward(q - 1).wait_recv()
                    pass_down(0, q - 1)
                    with jax.named_scope(f"share{q - 1}"):
                        share_far(q - 1).wait_recv()
                    pass_down(1, q - 1)
                if q == 5:
                    with jax.named_scope("arrive0"):
                        arrivals_down(0)
                if q >= 5:
                    hop_to(0, order[q - 5])
            with jax.named_scope("arrive1"):
                arrivals_down(1)

        @pl.when(core == 1)
        def _():
            for q in range(CHUNKS + 1):
                if q < CHUNKS:
                    with jax.named_scope(f"near{q}"):
                        to_near(q).wait_recv()
                    forward(q).start()
                if q >= 1:
                    with jax.named_scope(f"far{q - 1}"):
                        forward(q - 1).wait_recv()
                    share_far(q - 1).start()
                if q < CHUNKS:
                    with jax.named_scope(f"share{q}"):
                        share_near(q).wait_recv()
                    for start, count in GROUPS.get(q, ()):
                        pass_up(start, count)
            with jax.named_scope("arrive0"):
                arrivals_up(0)
            for k in order:
                hop_to(0, k)
            with jax.named_scope("arrive1"):
                arrivals_up(1)

        for k in order:
            hop_to(1, k)

        @pl.when(step == 1)
        def _():
            first_numbers()

        for part in range(PARTS):
            for k in range(1, RING):
                own_copy(own, part, k).wait_send()
        to_sibling.wait_send()
        for q in range(CHUNKS):
            to_near(q).wait_send()
            forward(q).wait_send()

        @pl.when(core == 0)
        def _():
            for q in range(CHUNKS):
                share_near(q).wait_send()
                for of in range(2):
                    p, copy = late_down(of, q)

                    @pl.when(p != r)
                    def _():
                        copy.wait_send()

        @pl.when(core == 1)
        def _():
            for q in range(CHUNKS):
                share_far(q).wait_send()
            for groups in GROUPS.values():
                for start, count in groups:
                    for part in range(PARTS):
                        for k in range(1, RING):
                            late_up(start, count, part, k).wait_send()

        pl.semaphore_signal(ready_sem, inc=1, device_id=sibling, device_id_type=MESH)

        @pl.when(step == 0)
        def _():
            for to in greeted:
                pl.semaphore_signal(free_sem, inc=1, device_id=to, device_id_type=MESH)

        with jax.named_scope("back"):
            for part in range(PARTS):
                for k in range(1, RING):
                    back_copy(part, k).wait()
        with jax.named_scope("ready"):
            pl.semaphore_wait(ready_sem, 1)

        def work_through(side_of, block):
            for t in range(per_piece):
                if side_of:
                    turn_tile(returned, turned, t, per_piece)
                swap(block, t, side_of).start()

            @pl.when(step == 0)
            def _():
                with jax.named_scope("work0"):
                    each_block(side_of, block, first_work, True)
                sum_start(0)

            @pl.when(step == 1)
            def _():
                with jax.named_scope("work1"):
                    each_block(side_of, block, second_sums, True)
                sum_start(1)
                with jax.named_scope("sum"):
                    sum_middle(1)
                    last_numbers()
                with jax.named_scope("finish"):
                    each_block(side_of, block, finish, False)

            for t in range(per_piece):
                swap(block, t, side_of).wait_send()

        @pl.when(core == 0)
        def _():
            work_through(0, returned)

        @pl.when(core == 1)
        def _():
            work_through(1, turned)

        @pl.when(step == 0)
        def _():
            with jax.named_scope("free"):
                pl.semaphore_wait(free_sem, len(greeted))

        return carry

    lax.fori_loop(0, STEPS, one_step, 0)
    with jax.named_scope("out"):
        stores = []
        for t in range(per_piece):
            copy = pltpu.make_async_copy(
                hopped_kept.at[t], out_ref.at[:, pl.ds(t * TILE, TILE)], load_sem.at[t]
            )
            copy.start()
            stores.append(copy)
        for copy in stores:
            copy.wait()


def body(start_vector, hop_tiles, tile_columns, tile_signs, occupation):
    half, side = start_vector.shape
    tile_k = hop_tiles.shape[1]
    sites, dets = occupation.shape
    per_piece = side // TILE
    held = RING * per_piece
    quarter = side // RING
    piece = quarter // PARTS
    ups = lax.axis_size("up")
    downs = lax.axis_size("dn")
    occupied = occupation.astype(jnp.bfloat16)
    row_start = lax.axis_index("up") * half
    col_start = lax.axis_index("dn") * side
    rows = lax.dynamic_slice_in_dim(occupied, row_start, half, 1).T
    cols = lax.dynamic_slice_in_dim(occupied, col_start, side, 1)
    rows = jnp.pad(rows, ((0, 0), (0, TILE - sites)))
    cols = jnp.pad(cols, ((0, TILE - sites), (0, 0))).reshape(TILE, per_piece, TILE).transpose(1, 0, 2)
    share = jnp.sum(occupation, axis=1).astype(jnp.float32) / dets
    shift = jnp.broadcast_to(coupling * jnp.sum(share * share), (ROWS, TILE))

    anywhere = pl.BlockSpec(memory_space=pl.ANY)
    scalars = pl.BlockSpec(memory_space=pltpu.SMEM)
    vmem = pl.BlockSpec(memory_space=pltpu.VMEM)
    block = pltpu.VMEM((per_piece, side, TILE), jnp.bfloat16)
    half_block = pltpu.VMEM((per_piece, half, TILE), jnp.bfloat16)
    dma = pltpu.SemaphoreType.DMA
    final, numbers = pl.pallas_call(
        functools.partial(recurrence_kernel, tile_k),
        in_specs=[scalars, scalars, anywhere, anywhere, vmem, vmem, vmem],
        out_specs=[anywhere, vmem],
        out_shape=[
            jax.ShapeDtypeStruct(start_vector.shape, jnp.bfloat16),
            jax.ShapeDtypeStruct((ROWS, TILE), jnp.float32),
        ],
        scratch_shapes=[
            block,
            block,
            block,
            block,
            block,
            pltpu.VMEM((2 * held, piece, TILE), jnp.bfloat16),
            pltpu.VMEM((2 * held, piece, TILE), jnp.bfloat16),
            pltpu.VMEM((PARTS, RING - 1, per_piece, piece, TILE), jnp.bfloat16),
            block,
            pltpu.VMEM((held, tile_k, TILE, TILE), jnp.bfloat16),
            half_block,
            half_block,
            pltpu.VMEM((3 * ROWS, TILE), jnp.float32),
            pltpu.VMEM((STEPS, downs, 3 * ROWS, TILE), jnp.float32),
            pltpu.VMEM((STEPS, ups, 3 * ROWS, TILE), jnp.float32),
            pltpu.VMEM((ROWS, TILE), jnp.float32),
            dma((per_piece,)),
            dma,
            dma,
            dma,
            dma((CHUNKS,)),
            dma((CHUNKS,)),
            dma((CHUNKS,)),
            dma((CHUNKS,)),
            dma((CHUNKS,)),
            dma((CHUNKS,)),
            dma((PARTS, RING - 1)),
            dma((PARTS, RING - 1)),
            dma((len(GROUP_AT) * PARTS * RING,)),
            dma((len(GROUP_AT) * PARTS * RING,)),
            dma((PARTS, RING - 1)),
            dma((PARTS, RING - 1)),
            dma((per_piece,)),
            dma((per_piece,)),
            dma((STEPS, downs)),
            dma((STEPS, downs)),
            dma((STEPS, ups)),
            dma((STEPS, ups)),
            pltpu.SemaphoreType.REGULAR,
            pltpu.SemaphoreType.REGULAR,
        ],
        compiler_params=pltpu.CompilerParams(
            collective_id=0, has_side_effects=True, vmem_limit_bytes=67043328
        ),
        name="recurrence",
    )(tile_columns.reshape(-1), tile_signs.reshape(-1), start_vector, hop_tiles, rows, cols, shift)
    return (final, numbers[0:2, 0], numbers[2:4, 0])


def solution(mesh):
    placed = (P("up", "dn"), P(), P(), P(), P())
    return jax.shard_map(
        body, mesh=mesh, in_specs=placed, out_specs=(P("up", "dn"), P(), P()), check_vma=False
    )
```

```python
import functools

import jax
import jax.numpy as jnp
from jax import lax
from jax.experimental import pallas as pl
from jax.experimental.pallas import tpu as pltpu
from jax.sharding import PartitionSpec as P

STEPS = 2
RING = 4
TILE = 128
MESH = pl.DeviceIdType.MESH

coupling = 4.0


def place():
    u = lax.axis_index("up")
    d = lax.axis_index("dn")
    return u // 8, (u // 2) % 4, u % 2, d // 4, d % 4


def device(y_lo, x, core, y_hi, z):
    return (y_lo * 8 + x * 2 + core, y_hi * 4 + z)


PARTS = 2
CUTS = (112, 96)
CHUNKS = 8
LENT = 64
WIDTH = 7
TILES_OF = ((0, 7), (7, 6))
GROUPS = (
    {1: (0, 1), 3: (1, 2), 5: (3, 1), 6: (4, 1), 7: (5, 2)},
    {1: (7, 1), 3: (8, 1), 5: (9, 2), 6: (11, 1), 7: (12, 1)},
)
COUNT = 5
ROWS = 8
ORDER = (2, 1, 3, 0)


def recurrence_kernel(
    tile_k,
    columns_ref,
    signs_ref,
    x_ref,
    tiles_ref,
    occ_ref,
    out_ref,
    numbers_ref,
    own,
    near,
    far,
    turned,
    turned_near,
    gathered_a,
    gathered_b,
    result,
    back_down,
    back_up,
    hopped_up,
    weights,
    kept,
    hopped_kept,
    occ_all,
    occ_rows,
    occ_cols,
    shift_ref,
    sums,
    first,
    second,
    factors,
    load_sem,
    tiles_sem,
    occ_sem,
    near_send,
    near_recv,
    far_send,
    far_recv,
    lend_send,
    lend_recv,
    own_down_send,
    own_down_recv,
    own_up_send,
    own_up_recv,
    late_down_send,
    late_down_recv,
    late_up_send,
    late_up_recv,
    back_down_send,
    back_down_recv,
    back_up_send,
    back_up_recv,
    down_send,
    down_recv,
    up_send,
    up_recv,
    free_sem,
):
    half, side = x_ref.shape
    sites, dets = occ_ref.shape
    quarter = side // RING
    piece = quarter // PARTS
    per_piece = side // TILE
    held = RING * per_piece
    gathered = (gathered_a, gathered_b)
    y_lo, x, core, y_hi, z = place()
    u = lax.axis_index("up")
    d = lax.axis_index("dn")
    ups = lax.axis_size("up")
    downs = lax.axis_size("dn")
    sibling = device(y_lo, x, 1 - core, y_hi, z)
    near_chip = device(1 - y_lo, x, core, y_hi, z)
    far_chip = device(1 - y_lo, x, core, 1 - y_hi, z)

    def remote(src, dst, send, recv, to):
        return pltpu.make_async_remote_copy(
            src_ref=src, dst_ref=dst, send_sem=send, recv_sem=recv, device_id=to, device_id_type=MESH
        )

    starts = [(q // 2) * piece + (q % 2) * CUTS[0] for q in range(CHUNKS)]
    sizes = [CUTS[q % 2] for q in range(CHUNKS)]

    def chip_rows(p, part):
        start = (p // 2) * half + (p % 2) * piece + part * quarter
        return pl.ds(pl.multiple_of(start, 16), piece)

    def half_rows(p, part):
        start = (p % 2) * piece + part * quarter
        return pl.ds(pl.multiple_of(start, 16), piece)

    barrier = pltpu.get_barrier_semaphore()
    partners = [sibling, near_chip, far_chip]
    for k in range(1, RING):
        for c in range(2):
            partners.append(device(y_lo, x, c, y_hi, (z + k) % RING))
            partners.append(device(y_lo, (x + k) % RING, c, y_hi, z))
    others = [device(y_lo, x, core, 1 - y_hi, (z + k) % RING) for k in range(RING)]
    others += [device(1 - y_lo, (x + k) % RING, core, y_hi, z) for k in range(1, RING)]
    others += [device(1 - y_lo, (x + k) % RING, 1 - core, y_hi, z) for k in range(RING)]
    for to in partners + others:
        pl.semaphore_signal(barrier, inc=1, device_id=to, device_id_type=MESH)

    loads = []
    for t in range(per_piece):
        copy = pltpu.make_async_copy(
            x_ref.at[:, pl.ds(t * TILE, TILE)], own.at[t, pl.ds(0, half)], load_sem.at[t]
        )
        copy.start()
        loads.append(copy)
    hop_side = y_hi + core * (y_lo - y_hi)
    first_tile = pl.multiple_of(hop_side * held, held)
    load_tiles = pltpu.make_async_copy(tiles_ref.at[pl.ds(first_tile, held)], weights, tiles_sem)
    load_tiles.start()
    load_occ = pltpu.make_async_copy(occ_ref, occ_all, occ_sem)
    load_occ.start()
    with jax.named_scope("barrier"):
        pl.semaphore_wait(barrier, len(partners) + len(others))
    with jax.named_scope("load"):
        for copy in loads:
            copy.wait()

    down_slot = pl.ds((y_hi * RING + z) * per_piece, per_piece)
    late_down_slot = pl.ds(((1 - y_hi) * RING + z) * per_piece, per_piece)
    up_start = (y_lo * RING + x) * per_piece
    late_up_start = ((1 - y_lo) * RING + x) * per_piece

    def to_near(q):
        rows = pl.ds(starts[q], sizes[q])
        return remote(own.at[:, rows], near.at[:, rows], near_send.at[q], near_recv.at[q], near_chip)

    def forward(q):
        rows = pl.ds(starts[q], sizes[q])
        return remote(near.at[:, rows], far.at[:, rows], far_send.at[q], far_recv.at[q], far_chip)

    def lend(which):
        block = (own, near)[which]
        return remote(
            block.at[:, pl.ds(0, LENT)],
            block.at[:, pl.ds(half, LENT)],
            lend_send.at[which],
            lend_recv.at[which],
            sibling,
        )

    def own_down(p, part):
        at = part * RING + (p - z) % RING
        return remote(
            own.at[:, half_rows(p, part)],
            gathered[part].at[down_slot],
            own_down_send.at[at],
            own_down_recv.at[at],
            device(y_lo, x, 0, y_hi, p),
        )

    def late_down(p, part, sub):
        at = (part * 2 + sub) * RING + (p - z) % RING
        start = (p % 2) * piece + part * quarter + sub * CUTS[0]
        return remote(
            far.at[:, pl.ds(pl.multiple_of(start, 16), CUTS[sub])],
            gathered[part].at[late_down_slot, pl.ds(sub * CUTS[0], CUTS[sub])],
            late_down_send.at[at],
            late_down_recv.at[at],
            device(y_lo, x, 0, y_hi, p),
        )

    def own_up(c, part, k):
        p = (x + k) % RING
        tile, count = TILES_OF[c]
        at = (c * PARTS + part) * RING + k
        return remote(
            turned.at[pl.ds(0, count), chip_rows(p, part)],
            gathered[part].at[pl.ds(up_start + tile, count)],
            own_up_send.at[at],
            own_up_recv.at[at],
            device(y_lo, p, 1, y_hi, z),
        )

    def late_up(c, group, part, k):
        p = (x + k) % RING
        tile, count = group
        number = list(GROUPS[c].values()).index(group)
        at = ((c * COUNT + number) * PARTS + part) * RING + k
        return remote(
            turned_near.at[pl.ds(tile - TILES_OF[c][0], count), chip_rows(p, part)],
            gathered[part].at[pl.ds(late_up_start + tile, count)],
            late_up_send.at[at],
            late_up_recv.at[at],
            device(y_lo, p, 1, y_hi, z),
        )

    def result_down(part, k):
        at = part * RING + k
        return remote(
            result.at[part, k],
            back_down.at[:, half_rows(z, part)],
            back_down_send.at[at],
            back_down_recv.at[at],
            device(y_lo, x, z // 2, y_hi, (z + k) % RING),
        )

    def result_up(part, k, c):
        at = part * RING + k
        return remote(
            result.at[part, k, pl.ds(c * (per_piece - WIDTH), WIDTH)],
            back_up.at[:, chip_rows(x, part)],
            back_up_send.at[c, at],
            back_up_recv.at[at],
            device(y_lo, (x + k) % RING, c, y_hi, z),
        )

    def turn_tile(c, source, target, i):
        top = i * TILE - c * half
        for j in range(per_piece):
            target[i - TILES_OF[c][0], j * TILE : (j + 1) * TILE, :] = source[j, top : top + TILE, :].T

    def hop_piece(part, p, target):
        def one_tile(t, carry):
            i = p * per_piece + t
            picked = []
            values = []
            for k in range(tile_k):
                picked.append(gathered[part][columns_ref[hop_side * held + i, k]])
                sign = (1 - 2 * signs_ref[hop_side * held + i, k]).astype(jnp.float32)
                values.append((weights[i, k].astype(jnp.float32) * sign).astype(jnp.bfloat16))
            left = jnp.concatenate(picked, axis=1)
            right = jnp.concatenate(values, axis=1)
            hopped = lax.dot_general(
                left, right, (((1,), (1,)), ((), ())), preferred_element_type=jnp.float32
            )
            target[t] = hopped.astype(jnp.bfloat16)
            return carry

        lax.fori_loop(0, per_piece, one_tile, 0)

    def hop_to(c, part, k):
        with jax.named_scope(f"hop{part}{k}"):
            if c == 0:
                hop_piece(part, (z + k) % RING, result.at[part, k])
                if k:
                    result_down(part, k).start()
                else:

                    @pl.when(z // 2 == 1)
                    def _():
                        result_down(part, 0).start()

                    @pl.when(z // 2 == 0)
                    def _():
                        back_down[:, half_rows(z, part)] = result[part, 0]
            else:
                hop_piece(part, (x + k) % RING, result.at[part, k])
                result_up(part, k, 0).start()
                if k:
                    result_up(part, k, 1).start()
                else:
                    back_up[:, chip_rows(x, part)] = result[part, 0, per_piece - WIDTH :]

    def arrive(c, part):
        if c == 0:
            for k in range(1, RING):
                own_down((z + k) % RING, part).wait_recv()
                for sub in range(2):
                    late_down((z + k) % RING, part, sub).wait_recv()

            @pl.when(z // 2 == 1)
            def _():
                own_down(z, part).wait_recv()
                for sub in range(2):
                    late_down(z, part, sub).wait_recv()
        else:
            for side_of in range(2):
                for k in range(side_of, RING):
                    own_up(side_of, part, k).wait_recv()
                    for group in GROUPS[side_of].values():
                        late_up(side_of, group, part, k).wait_recv()

    def sum_down(use, j):
        return remote(
            first.at[use, d], first.at[use, d], down_send.at[use, j], down_recv.at[use, j], (u, (d + j) % downs)
        )

    def sum_up(use, j):
        return remote(
            second.at[use, u], second.at[use, u], up_send.at[use, j], up_recv.at[use, j], ((u + j) % ups, d)
        )

    def sum_start(use):
        first[use, d] = sums[...]
        for j in range(1, downs):
            sum_down(use, j).start()

    def sum_middle(use):
        for j in range(1, downs):
            sum_down(use, j).wait()
        total = first[use, 0]
        for j in range(1, downs):
            total = total + first[use, j]
        second[use, u] = total
        for j in range(1, ups):
            sum_up(use, j).start()

    def sum_end(use):
        for j in range(1, ups):
            sum_up(use, j).wait()
        total = second[use, 0]
        for j in range(1, ups):
            total = total + second[use, j]
        parts = [total[ROWS * i : ROWS * (i + 1)] for i in range(3)]
        return [jnp.sum(jnp.sum(part, axis=0, keepdims=True), axis=1, keepdims=True) for part in parts]

    def keep_factor(row, value):
        factors[row : row + 1, :] = jnp.broadcast_to(value, (1, TILE))

    def first_numbers():
        total, cross, square = sum_end(0)
        shift = shift_ref[0:1, 0:1]
        scale = 1.0 / jnp.maximum(jnp.sqrt(total), 1.0)
        alpha = scale * scale * (cross + shift * total)
        delta = alpha - shift
        residual = scale * scale * (square - 2.0 * delta * cross + delta * delta * total)
        beta = jnp.sqrt(jnp.maximum(residual, 1.0))
        keep_factor(0, delta)
        keep_factor(1, scale / beta)
        keep_factor(2, beta * scale)
        keep_factor(3, alpha)
        keep_factor(4, beta)

    def last_numbers():
        total, cross, square = sum_end(1)
        shift = shift_ref[0:1, 0:1]
        alpha = cross + shift * total
        delta = alpha - shift
        residual = square - 2.0 * delta * cross + delta * delta * total
        beta = jnp.sqrt(jnp.maximum(residual, 1.0))
        keep_factor(5, delta)
        keep_factor(6, 1.0 / beta)
        numbers_ref[...] = jnp.zeros_like(numbers_ref)
        numbers_ref[0:1, :] = factors[3:4, :]
        numbers_ref[1:2, :] = jnp.broadcast_to(alpha, (1, TILE))
        numbers_ref[2:3, :] = factors[4:5, :]
        numbers_ref[3:4, :] = jnp.broadcast_to(beta, (1, TILE))

    def prepare_diagonal():
        load_occ.wait()
        blank = jnp.zeros((TILE - sites, TILE), jnp.bfloat16)
        row_base = (y_lo * RING + x) * side
        col_base = d * side

        def one_block(j, carry):
            for base, turn, target in ((row_base, True, occ_rows), (col_base, False, occ_cols)):
                lanes = pl.ds(pl.multiple_of(base + j * TILE, TILE), TILE)
                found = occ_all[:, lanes].astype(jnp.float32).astype(jnp.bfloat16)
                filled = jnp.concatenate([found, blank], axis=0)
                target[j] = filled.T if turn else filled
            return carry

        lax.fori_loop(0, per_piece, one_block, 0)

        def add_tile(j, carry):
            return carry + occ_all[:, pl.ds(pl.multiple_of(j * TILE, TILE), TILE)]

        counts = lax.fori_loop(0, dets // TILE, add_tile, jnp.zeros((sites, TILE), jnp.int32))
        share = jnp.sum(counts.astype(jnp.float32), axis=1, keepdims=True) * (1.0 / dets)
        mean = coupling * jnp.sum(share * share, axis=0, keepdims=True)
        shift_ref[...] = jnp.broadcast_to(mean, shift_ref.shape)

    def fold(value):
        return jnp.sum(value.reshape(-1, ROWS, TILE), axis=0)

    blocks = [(a * TILE, min(TILE, half - a * TILE)) for a in range(WIDTH)]

    def each_block(c, act, count=3):
        def one_tile(t, totals):
            totals = list(totals)
            for start, size in blocks:
                rows = slice(start, start + size)
                top = c * half + start
                tops = [(top // TILE, top % TILE, min(size, TILE - top % TILE))]
                if tops[0][2] < size:
                    tops.append((top // TILE + 1, 0, size - tops[0][2]))
                left = [occ_rows[i, low : low + n, :] for i, low, n in tops]
                left = left[0] if len(left) == 1 else jnp.concatenate(left, axis=0)
                offset = jnp.dot(left, occ_cols[t], preferred_element_type=jnp.float32)
                offset = coupling * offset - shift_ref[0:1, :]
                lifted = slice(c * LENT + start, c * LENT + start + size)
                found = act(t, rows, lifted, offset)
                if found is not None:
                    totals = [total + fold(value) for total, value in zip(totals, found)]
            return tuple(totals)

        zero = jnp.zeros((ROWS, TILE), jnp.float32)
        return lax.fori_loop(0, per_piece, one_tile, (zero,) * count)

    def both_hops(t, rows, lifted):
        return back_down[t, rows].astype(jnp.float32) + hopped_up[t, lifted].astype(jnp.float32)

    def first_work(t, rows, lifted, offset):
        hopped = both_hops(t, rows, lifted)
        start = own[t, rows]
        kept[t, rows] = start
        hopped_kept[t, rows] = hopped.astype(jnp.bfloat16)
        start = start.astype(jnp.float32)
        work = hopped + offset * start
        own[t, rows] = work.astype(jnp.bfloat16)
        return start * start, work * start, work * work

    def held_vector(t, rows):
        start = kept[t, rows].astype(jnp.float32)
        return start, own[t, rows].astype(jnp.float32) - factors[0:1, :] * start

    def second_work(t, rows, lifted, offset):
        delta, gain, push = factors[0:1, :], factors[1:2, :], factors[2:3, :]
        hopped = both_hops(t, rows, lifted)
        start, before = held_vector(t, rows)
        vector = gain * before
        held_hop = hopped_kept[t, rows].astype(jnp.float32)
        work = gain * (hopped - delta * held_hop + offset * before) - push * start
        high = work.astype(jnp.bfloat16)
        near[t, rows] = high
        far[t, rows] = (work - high.astype(jnp.float32)).astype(jnp.bfloat16)
        return vector * vector, work * vector, work * work

    def finish():
        def one_tile(t, carry):
            for start, size in blocks:
                rows = slice(start, start + size)
                work = near[t, rows].astype(jnp.float32) + far[t, rows].astype(jnp.float32)
                _, before = held_vector(t, rows)
                final = (work - factors[5:6, :] * factors[1:2, :] * before) * factors[6:7, :]
                hopped_kept[t, rows] = final.astype(jnp.bfloat16)
            return carry

        lax.fori_loop(0, per_piece, one_tile, 0)

    def send_down(c, p, copy, copy_self):
        if c == 0:

            @pl.when(p != z)
            def _():
                copy.start()

            @pl.when(p == z)
            def _():
                copy_self()
        else:
            copy.start()

    def down_sent(c, p, copy):
        if c == 0:

            @pl.when(p != z)
            def _():
                copy.wait_send()
        else:
            copy.wait_send()

    def up_range(c):
        return range(c, RING)

    def one_step(c, step, carry):
        for q in range(CHUNKS):
            to_near(q).start()
        if c == 1:
            lend(0).start()
        for part in range(PARTS):
            for p in (2 * c, 2 * c + 1):

                def copy_self(p=p, part=part):
                    gathered[part][down_slot] = own[:, half_rows(p, part)]

                send_down(c, p, own_down(p, part), copy_self)
        tile, count = TILES_OF[c]
        with jax.named_scope("turn_own"):
            for i in range(tile, tile + count):
                if c == 0 and i == tile + count - 1:
                    lend(0).wait_recv()
                turn_tile(c, own, turned, i)
        for part in range(PARTS):
            for k in (2, 1, 3):
                own_up(c, part, k).start()
            if c == 0:
                own_up(c, part, 0).start()
            else:
                gathered[part][pl.ds(up_start + tile, count)] = turned[:count, chip_rows(x, part)]

        @pl.when(step == 0)
        def _():
            with jax.named_scope("diagonal"):
                prepare_diagonal()
                load_tiles.wait()

        @pl.when(step == 1)
        def _():
            sum_middle(0)

        for q in range(CHUNKS + 1):
            if q < CHUNKS:
                with jax.named_scope(f"near{q}"):
                    to_near(q).wait_recv()
                forward(q).start()
                if q == 0 and c == 1:
                    lend(1).start()
            if q >= 1:
                with jax.named_scope(f"far{q - 1}"):
                    forward(q - 1).wait_recv()
                p, part, sub = 2 * c + ((q - 1) // 2) % 2, (q - 1) // 4, (q - 1) % 2

                def copy_self(part=part, sub=sub, q=q):
                    rows = slice(starts[q - 1], starts[q - 1] + sizes[q - 1])
                    gathered[part][late_down_slot, sub * CUTS[0] : sub * CUTS[0] + CUTS[sub]] = far[:, rows]

                send_down(c, p, late_down(p, part, sub), copy_self)
            if q in GROUPS[c]:
                group = GROUPS[c][q]
                for i in range(group[0], group[0] + group[1]):
                    if c == 0 and i == TILES_OF[0][1] - 1:
                        lend(1).wait_recv()
                    turn_tile(c, near, turned_near, i)
                for part in range(PARTS):
                    for k in (2, 1, 3):
                        late_up(c, group, part, k).start()
                    if c == 0:
                        late_up(c, group, part, 0).start()
                    else:
                        gathered[part][pl.ds(late_up_start + group[0], group[1])] = turned_near[
                            group[0] - tile : group[0] - tile + group[1], chip_rows(x, part)
                        ]
            if c == 0 and q == 5:
                with jax.named_scope("arrive0"):
                    arrive(c, 0)
            if c == 0 and q >= 5:
                hop_to(c, 0, ORDER[q - 5])
        if c == 1:
            with jax.named_scope("arrive0"):
                arrive(c, 0)
            for k in ORDER:
                hop_to(c, 0, k)
        with jax.named_scope("arrive1"):
            arrive(c, 1)
        for k in ORDER:
            hop_to(c, 1, k)

        @pl.when(step == 1)
        def _():
            first_numbers()

        for q in range(CHUNKS):
            to_near(q).wait_send()
            forward(q).wait_send()
        if c == 1:
            lend(0).wait_send()
            lend(1).wait_send()
        for part in range(PARTS):
            for p in (2 * c, 2 * c + 1):
                down_sent(c, p, own_down(p, part))
                for sub in range(2):
                    down_sent(c, p, late_down(p, part, sub))
            for k in up_range(c):
                own_up(c, part, k).wait_send()
                for group in GROUPS[c].values():
                    late_up(c, group, part, k).wait_send()

        @pl.when(step == 0)
        def _():
            for to in partners:
                pl.semaphore_signal(free_sem, inc=1, device_id=to, device_id_type=MESH)

        with jax.named_scope("back_up"):
            for part in range(PARTS):
                for k in range(c, RING):
                    result_up(part, k, c).wait_recv()
        with jax.named_scope("turn_back"):
            for t in range(per_piece):
                for i in range(WIDTH):
                    hopped_up[t, i * TILE : (i + 1) * TILE, :] = back_up[i, t * TILE : (t + 1) * TILE, :].T
        with jax.named_scope("back_down"):
            for part in range(PARTS):
                for source in (2 * c, 2 * c + 1):
                    k = (z - source) % RING
                    copy = remote(
                        result.at[part, 0],
                        back_down.at[:, half_rows(source, part)],
                        back_down_send.at[part * RING],
                        back_down_recv.at[part * RING + k],
                        sibling,
                    )
                    if c == 0:

                        @pl.when(source != z)
                        def _():
                            copy.wait_recv()
                    else:
                        copy.wait_recv()
        for part in range(PARTS):
            for k in range(RING):
                if c == 0:
                    if k:
                        result_down(part, k).wait_send()
                    else:

                        @pl.when(z // 2 == 1)
                        def _():
                            result_down(part, 0).wait_send()
                else:
                    result_up(part, k, 0).wait_send()
                    if k:
                        result_up(part, k, 1).wait_send()

        def store_sums(found):
            for i, value in enumerate(found):
                sums[ROWS * i : ROWS * (i + 1), :] = value

        @pl.when(step == 0)
        def _():
            with jax.named_scope("work0"):
                store_sums(each_block(c, first_work))
            sum_start(0)
            with jax.named_scope("free"):
                pl.semaphore_wait(free_sem, len(partners))

        @pl.when(step == 1)
        def _():
            with jax.named_scope("work1"):
                store_sums(each_block(c, second_work))
            sum_start(1)
            with jax.named_scope("sum"):
                sum_middle(1)
                last_numbers()
            with jax.named_scope("finish"):
                finish()

        return carry

    for c in range(2):

        @pl.when(core == c)
        def _(c=c):
            lax.fori_loop(0, STEPS, functools.partial(one_step, c), 0)

    with jax.named_scope("out"):
        stores = []
        for t in range(per_piece):
            copy = pltpu.make_async_copy(
                hopped_kept.at[t], out_ref.at[:, pl.ds(t * TILE, TILE)], load_sem.at[t]
            )
            copy.start()
            stores.append(copy)
        for copy in stores:
            copy.wait()


def body(start_vector, hop_tiles, tile_columns, tile_signs, occupation):
    half, side = start_vector.shape
    tile_k = hop_tiles.shape[1]
    per_piece = side // TILE
    held = RING * per_piece
    quarter = side // RING
    piece = quarter // PARTS
    ups = lax.axis_size("up")
    downs = lax.axis_size("dn")

    anywhere = pl.BlockSpec(memory_space=pl.ANY)
    scalars = pl.BlockSpec(memory_space=pltpu.SMEM)
    vmem = pl.BlockSpec(memory_space=pltpu.VMEM)
    dma = pltpu.SemaphoreType.DMA

    def bf16(*shape):
        return pltpu.VMEM(shape, jnp.bfloat16)

    def f32(*shape):
        return pltpu.VMEM(shape, jnp.float32)

    def pair(*shape):
        return [dma(shape), dma(shape)]

    final, numbers = pl.pallas_call(
        functools.partial(recurrence_kernel, tile_k),
        in_specs=[scalars, scalars, anywhere, anywhere, anywhere],
        out_specs=[anywhere, vmem],
        out_shape=[
            jax.ShapeDtypeStruct(start_vector.shape, jnp.bfloat16),
            jax.ShapeDtypeStruct((ROWS, TILE), jnp.float32),
        ],
        scratch_shapes=[
            bf16(per_piece, half + LENT, TILE),
            bf16(per_piece, half + LENT, TILE),
            bf16(per_piece, half, TILE),
            bf16(WIDTH, side, TILE),
            bf16(WIDTH, side, TILE),
            bf16(2 * held, piece, TILE),
            bf16(2 * held, piece, TILE),
            bf16(PARTS, RING, per_piece, piece, TILE),
            bf16(per_piece, half, TILE),
            bf16(WIDTH, side, TILE),
            bf16(per_piece, half + LENT, TILE),
            bf16(held, tile_k, TILE, TILE),
            bf16(per_piece, half, TILE),
            bf16(per_piece, half, TILE),
            pltpu.VMEM(occupation.shape, jnp.int32),
            bf16(per_piece, TILE, TILE),
            bf16(per_piece, TILE, TILE),
            f32(ROWS, TILE),
            f32(3 * ROWS, TILE),
            f32(STEPS, downs, 3 * ROWS, TILE),
            f32(STEPS, ups, 3 * ROWS, TILE),
            f32(ROWS, TILE),
            dma((per_piece,)),
            dma,
            dma,
            *pair(CHUNKS),
            *pair(CHUNKS),
            *pair(2),
            *pair(PARTS * RING),
            *pair(2 * PARTS * RING),
            *pair(2 * PARTS * RING),
            *pair(2 * COUNT * PARTS * RING),
            *pair(PARTS * RING),
            dma((2, PARTS * RING)),
            dma((PARTS * RING,)),
            *pair(STEPS, downs),
            *pair(STEPS, ups),
            pltpu.SemaphoreType.REGULAR,
        ],
        compiler_params=pltpu.CompilerParams(
            collective_id=0, has_side_effects=True, vmem_limit_bytes=67043328
        ),
        name="recurrence",
    )(tile_columns, tile_signs, start_vector, hop_tiles, occupation)
    return (final, numbers[0:2, 0], numbers[2:4, 0])


def solution(mesh):
    placed = (P("up", "dn"), P(), P(), P(), P())
    return jax.shard_map(
        body, mesh=mesh, in_specs=placed, out_specs=(P("up", "dn"), P(), P()), check_vma=False
    )
```

```python
import functools

import jax
import jax.numpy as jnp
from jax import lax
from jax.experimental import pallas as pl
from jax.experimental.pallas import tpu as pltpu
from jax.sharding import PartitionSpec as P

STEPS = 2
RING = 4
TILE = 128
MESH = pl.DeviceIdType.MESH

coupling = 4.0


def place():
    u = lax.axis_index("up")
    d = lax.axis_index("dn")
    return u // 8, (u // 2) % 4, u % 2, d // 4, d % 4


def device(y_lo, x, core, y_hi, z):
    return (y_lo * 8 + x * 2 + core, y_hi * 4 + z)


PARTS = 2
CUTS = (112, 96)
CHUNKS = 8
LENT = 64
WIDTH = 7
TILES_OF = ((0, 7), (7, 6))
GROUPS = (
    {1: (0, 1), 3: (1, 2), 5: (3, 1), 6: (4, 1), 7: (5, 2)},
    {1: (7, 1), 3: (8, 1), 5: (9, 2), 6: (11, 1), 7: (12, 1)},
)
COUNT = 5
ROWS = 8
GROUP = 2
ORDER = (2, 1, 3, 0)


def recurrence_kernel(
    tile_k,
    lists_ref,
    x_ref,
    tiles_ref,
    occ_ref,
    out_ref,
    numbers_ref,
    own,
    near,
    far,
    turned,
    turned_near,
    gathered_a,
    gathered_b,
    result,
    back_down,
    back_up,
    hopped_up,
    weights,
    kept,
    hopped_kept,
    occ_all,
    occ_rows,
    occ_cols,
    shift_ref,
    sums,
    first,
    second,
    factors,
    load_sem,
    tiles_sem,
    occ_sem,
    near_send,
    near_recv,
    far_send,
    far_recv,
    lend_send,
    lend_recv,
    own_down_send,
    own_down_recv,
    own_up_send,
    own_up_recv,
    late_down_send,
    late_down_recv,
    late_up_send,
    late_up_recv,
    back_down_send,
    back_down_recv,
    back_up_send,
    back_up_recv,
    down_send,
    down_recv,
    up_send,
    up_recv,
    free_sem,
):
    half, side = x_ref.shape
    sites, dets = occ_ref.shape
    quarter = side // RING
    piece = quarter // PARTS
    per_piece = side // TILE
    held = RING * per_piece
    gathered = (gathered_a, gathered_b)
    y_lo, x, core, y_hi, z = place()
    u = lax.axis_index("up")
    d = lax.axis_index("dn")
    ups = lax.axis_size("up")
    downs = lax.axis_size("dn")
    sibling = device(y_lo, x, 1 - core, y_hi, z)
    near_chip = device(1 - y_lo, x, core, y_hi, z)
    far_chip = device(1 - y_lo, x, core, 1 - y_hi, z)

    def remote(src, dst, send, recv, to):
        return pltpu.make_async_remote_copy(
            src_ref=src, dst_ref=dst, send_sem=send, recv_sem=recv, device_id=to, device_id_type=MESH
        )

    starts = [(q // 2) * piece + (q % 2) * CUTS[0] for q in range(CHUNKS)]
    sizes = [CUTS[q % 2] for q in range(CHUNKS)]

    def chip_rows(p, part):
        start = (p // 2) * half + (p % 2) * piece + part * quarter
        return pl.ds(pl.multiple_of(start, 16), piece)

    def half_rows(p, part):
        start = (p % 2) * piece + part * quarter
        return pl.ds(pl.multiple_of(start, 16), piece)

    barrier = pltpu.get_barrier_semaphore()
    partners = [sibling, near_chip, far_chip]
    for k in range(1, RING):
        for c in range(2):
            partners.append(device(y_lo, x, c, y_hi, (z + k) % RING))
            partners.append(device(y_lo, (x + k) % RING, c, y_hi, z))
    others = [device(y_lo, x, core, 1 - y_hi, (z + k) % RING) for k in range(RING)]
    others += [device(1 - y_lo, (x + k) % RING, core, y_hi, z) for k in range(1, RING)]
    others += [device(1 - y_lo, (x + k) % RING, 1 - core, y_hi, z) for k in range(RING)]
    for to in partners + others:
        pl.semaphore_signal(barrier, inc=1, device_id=to, device_id_type=MESH)

    loads = []
    for t in range(per_piece):
        copy = pltpu.make_async_copy(
            x_ref.at[:, pl.ds(t * TILE, TILE)], own.at[t, pl.ds(0, half)], load_sem.at[t]
        )
        copy.start()
        loads.append(copy)
    hop_side = y_hi + core * (y_lo - y_hi)
    first_tile = pl.multiple_of(hop_side * held, held)
    load_tiles = pltpu.make_async_copy(tiles_ref.at[pl.ds(first_tile, held)], weights, tiles_sem)
    load_tiles.start()
    load_occ = pltpu.make_async_copy(occ_ref, occ_all, occ_sem)
    load_occ.start()
    with jax.named_scope("barrier"):
        pl.semaphore_wait(barrier, len(partners) + len(others))
    with jax.named_scope("load"):
        for copy in loads:
            copy.wait()

    down_slot = pl.ds((y_hi * RING + z) * per_piece, per_piece)
    late_down_slot = pl.ds(((1 - y_hi) * RING + z) * per_piece, per_piece)
    up_start = (y_lo * RING + x) * per_piece
    late_up_start = ((1 - y_lo) * RING + x) * per_piece

    def to_near(q):
        rows = pl.ds(starts[q], sizes[q])
        return remote(own.at[:, rows], near.at[:, rows], near_send.at[q], near_recv.at[q], near_chip)

    def forward(q):
        rows = pl.ds(starts[q], sizes[q])
        return remote(near.at[:, rows], far.at[:, rows], far_send.at[q], far_recv.at[q], far_chip)

    def lend(which):
        block = (own, near)[which]
        return remote(
            block.at[:, pl.ds(0, LENT)],
            block.at[:, pl.ds(half, LENT)],
            lend_send.at[which],
            lend_recv.at[which],
            sibling,
        )

    def own_down(p, part):
        at = part * RING + (p - z) % RING
        return remote(
            own.at[:, half_rows(p, part)],
            gathered[part].at[down_slot],
            own_down_send.at[at],
            own_down_recv.at[at],
            device(y_lo, x, 0, y_hi, p),
        )

    def late_down(p, part, sub):
        at = (part * 2 + sub) * RING + (p - z) % RING
        start = (p % 2) * piece + part * quarter + sub * CUTS[0]
        return remote(
            far.at[:, pl.ds(pl.multiple_of(start, 16), CUTS[sub])],
            gathered[part].at[late_down_slot, pl.ds(sub * CUTS[0], CUTS[sub])],
            late_down_send.at[at],
            late_down_recv.at[at],
            device(y_lo, x, 0, y_hi, p),
        )

    def own_up(c, part, k):
        p = (x + k) % RING
        tile, count = TILES_OF[c]
        at = (c * PARTS + part) * RING + k
        return remote(
            turned.at[pl.ds(0, count), chip_rows(p, part)],
            gathered[part].at[pl.ds(up_start + tile, count)],
            own_up_send.at[at],
            own_up_recv.at[at],
            device(y_lo, p, 1, y_hi, z),
        )

    def late_up(c, group, part, k):
        p = (x + k) % RING
        tile, count = group
        number = list(GROUPS[c].values()).index(group)
        at = ((c * COUNT + number) * PARTS + part) * RING + k
        return remote(
            turned_near.at[pl.ds(tile - TILES_OF[c][0], count), chip_rows(p, part)],
            gathered[part].at[pl.ds(late_up_start + tile, count)],
            late_up_send.at[at],
            late_up_recv.at[at],
            device(y_lo, p, 1, y_hi, z),
        )

    def result_down(part, k):
        at = part * RING + k
        return remote(
            result.at[part, k],
            back_down.at[:, half_rows(z, part)],
            back_down_send.at[at],
            back_down_recv.at[at],
            device(y_lo, x, z // 2, y_hi, (z + k) % RING),
        )

    def result_up(part, k, c):
        at = part * RING + k
        return remote(
            result.at[part, k, pl.ds(c * (per_piece - WIDTH), WIDTH)],
            back_up.at[:, chip_rows(x, part)],
            back_up_send.at[c, at],
            back_up_recv.at[at],
            device(y_lo, (x + k) % RING, c, y_hi, z),
        )

    def turn_tile(c, source, target, i):
        top = i * TILE - c * half
        for j in range(per_piece):
            target[i - TILES_OF[c][0], j * TILE : (j + 1) * TILE, :] = source[j, top : top + TILE, :].T

    def hop_piece(part, p, target):
        def one_tile(t):
            i = p * per_piece + t
            picked = [gathered[part][lists_ref[hop_side * held + i, k]] for k in range(tile_k)]
            values = [weights[i, k] for k in range(tile_k)]
            left = jnp.concatenate(picked, axis=1)
            right = jnp.concatenate(values, axis=0)
            return jnp.dot(left, right, preferred_element_type=jnp.float32).astype(jnp.bfloat16)

        def some_tiles(j, carry):
            found = [one_tile(j * GROUP + n) for n in range(GROUP)]
            for n in range(GROUP):
                target[j * GROUP + n] = found[n]
            return carry

        lax.fori_loop(0, per_piece // GROUP, some_tiles, 0)
        for t in range(per_piece // GROUP * GROUP, per_piece):
            target[t] = one_tile(t)

    def hop_to(c, part, k):
        with jax.named_scope(f"hop{part}{k}"):
            if c == 0:
                hop_piece(part, (z + k) % RING, result.at[part, k])
                if k:
                    result_down(part, k).start()
                else:

                    @pl.when(z // 2 == 1)
                    def _():
                        result_down(part, 0).start()

                    @pl.when(z // 2 == 0)
                    def _():
                        back_down[:, half_rows(z, part)] = result[part, 0]
            else:
                hop_piece(part, (x + k) % RING, result.at[part, k])
                result_up(part, k, 0).start()
                if k:
                    result_up(part, k, 1).start()
                else:
                    back_up[:, chip_rows(x, part)] = result[part, 0, per_piece - WIDTH :]

    def arrive(c, part):
        if c == 0:
            for k in range(1, RING):
                own_down((z + k) % RING, part).wait_recv()
                for sub in range(2):
                    late_down((z + k) % RING, part, sub).wait_recv()

            @pl.when(z // 2 == 1)
            def _():
                own_down(z, part).wait_recv()
                for sub in range(2):
                    late_down(z, part, sub).wait_recv()
        else:
            for side_of in range(2):
                for k in range(side_of, RING):
                    own_up(side_of, part, k).wait_recv()
                    for group in GROUPS[side_of].values():
                        late_up(side_of, group, part, k).wait_recv()

    def prepare_tiles():
        load_tiles.wait()

        def one_row(i, carry):
            for k in range(tile_k):
                sign = (1 - 2 * lists_ref[2 * held + hop_side * held + i, k]).astype(jnp.float32)
                weights[i, k] = (weights[i, k].astype(jnp.float32) * sign).astype(jnp.bfloat16).T
            return carry

        lax.fori_loop(0, held, one_row, 0)

    def sum_down(use, j):
        return remote(
            first.at[use, d], first.at[use, d], down_send.at[use, j], down_recv.at[use, j], (u, (d + j) % downs)
        )

    def sum_up(use, j):
        return remote(
            second.at[use, u], second.at[use, u], up_send.at[use, j], up_recv.at[use, j], ((u + j) % ups, d)
        )

    def sum_start(use):
        first[use, d] = sums[...]
        for j in range(1, downs):
            sum_down(use, j).start()

    def sum_middle(use):
        for j in range(1, downs):
            sum_down(use, j).wait()
        total = first[use, 0]
        for j in range(1, downs):
            total = total + first[use, j]
        second[use, u] = total
        for j in range(1, ups):
            sum_up(use, j).start()

    def sum_end(use):
        for j in range(1, ups):
            sum_up(use, j).wait()
        total = second[use, 0]
        for j in range(1, ups):
            total = total + second[use, j]
        parts = [total[ROWS * i : ROWS * (i + 1)] for i in range(3)]
        return [jnp.sum(jnp.sum(part, axis=0, keepdims=True), axis=1, keepdims=True) for part in parts]

    def keep_factor(row, value):
        factors[row : row + 1, :] = jnp.broadcast_to(value, (1, TILE))

    def first_numbers():
        total, cross, square = sum_end(0)
        shift = shift_ref[0:1, 0:1]
        scale = 1.0 / jnp.maximum(jnp.sqrt(total), 1.0)
        alpha = scale * scale * (cross + shift * total)
        delta = alpha - shift
        residual = scale * scale * (square - 2.0 * delta * cross + delta * delta * total)
        beta = jnp.sqrt(jnp.maximum(residual, 1.0))
        keep_factor(0, delta)
        keep_factor(1, scale / beta)
        keep_factor(2, beta * scale)
        keep_factor(3, alpha)
        keep_factor(4, beta)

    def last_numbers():
        total, cross, square = sum_end(1)
        shift = shift_ref[0:1, 0:1]
        alpha = cross + shift * total
        delta = alpha - shift
        residual = square - 2.0 * delta * cross + delta * delta * total
        beta = jnp.sqrt(jnp.maximum(residual, 1.0))
        keep_factor(5, delta)
        keep_factor(6, 1.0 / beta)
        numbers_ref[...] = jnp.zeros_like(numbers_ref)
        numbers_ref[0:1, :] = factors[3:4, :]
        numbers_ref[1:2, :] = jnp.broadcast_to(alpha, (1, TILE))
        numbers_ref[2:3, :] = factors[4:5, :]
        numbers_ref[3:4, :] = jnp.broadcast_to(beta, (1, TILE))

    def prepare_diagonal():
        load_occ.wait()
        blank = jnp.zeros((TILE - sites, TILE), jnp.bfloat16)
        row_base = (y_lo * RING + x) * side
        col_base = d * side

        def one_block(j, carry):
            for base, turn, target in ((row_base, True, occ_rows), (col_base, False, occ_cols)):
                lanes = pl.ds(pl.multiple_of(base + j * TILE, TILE), TILE)
                found = occ_all[:, lanes].astype(jnp.float32).astype(jnp.bfloat16)
                filled = jnp.concatenate([found, blank], axis=0)
                target[j] = filled.T if turn else filled
            return carry

        lax.fori_loop(0, per_piece, one_block, 0)

        def add_tile(j, carry):
            return carry + occ_all[:, pl.ds(pl.multiple_of(j * TILE, TILE), TILE)]

        counts = lax.fori_loop(0, dets // TILE, add_tile, jnp.zeros((sites, TILE), jnp.int32))
        share = jnp.sum(counts.astype(jnp.float32), axis=1, keepdims=True) * (1.0 / dets)
        mean = coupling * jnp.sum(share * share, axis=0, keepdims=True)
        shift_ref[...] = jnp.broadcast_to(mean, shift_ref.shape)

    def fold(value):
        return jnp.sum(value.reshape(-1, ROWS, TILE), axis=0)

    blocks = [(a * TILE, min(TILE, half - a * TILE)) for a in range(WIDTH)]

    def each_block(c, act, count=3):
        def one_tile(t, totals):
            totals = list(totals)
            for start, size in blocks:
                rows = slice(start, start + size)
                top = c * half + start
                tops = [(top // TILE, top % TILE, min(size, TILE - top % TILE))]
                if tops[0][2] < size:
                    tops.append((top // TILE + 1, 0, size - tops[0][2]))
                left = [occ_rows[i, low : low + n, :] for i, low, n in tops]
                left = left[0] if len(left) == 1 else jnp.concatenate(left, axis=0)
                offset = jnp.dot(left, occ_cols[t], preferred_element_type=jnp.float32)
                offset = coupling * offset - shift_ref[0:1, :]
                lifted = slice(c * LENT + start, c * LENT + start + size)
                found = act(t, rows, lifted, offset)
                if found is not None:
                    totals = [total + fold(value) for total, value in zip(totals, found)]
            return tuple(totals)

        zero = jnp.zeros((ROWS, TILE), jnp.float32)
        return lax.fori_loop(0, per_piece, one_tile, (zero,) * count)

    def both_hops(t, rows, lifted):
        return back_down[t, rows].astype(jnp.float32) + hopped_up[t, lifted].astype(jnp.float32)

    def first_work(t, rows, lifted, offset):
        hopped = both_hops(t, rows, lifted)
        start = own[t, rows]
        kept[t, rows] = start
        hopped_kept[t, rows] = hopped.astype(jnp.bfloat16)
        start = start.astype(jnp.float32)
        work = hopped + offset * start
        own[t, rows] = work.astype(jnp.bfloat16)
        return start * start, work * start, work * work

    def held_vector(t, rows):
        start = kept[t, rows].astype(jnp.float32)
        return start, own[t, rows].astype(jnp.float32) - factors[0:1, :] * start

    def second_work(t, rows, lifted, offset):
        delta, gain, push = factors[0:1, :], factors[1:2, :], factors[2:3, :]
        hopped = both_hops(t, rows, lifted)
        start, before = held_vector(t, rows)
        vector = gain * before
        held_hop = hopped_kept[t, rows].astype(jnp.float32)
        work = gain * (hopped - delta * held_hop + offset * before) - push * start
        high = work.astype(jnp.bfloat16)
        near[t, rows] = high
        far[t, rows] = (work - high.astype(jnp.float32)).astype(jnp.bfloat16)
        return vector * vector, work * vector, work * work

    def finish():
        def one_tile(t, carry):
            for start, size in blocks:
                rows = slice(start, start + size)
                work = near[t, rows].astype(jnp.float32) + far[t, rows].astype(jnp.float32)
                _, before = held_vector(t, rows)
                final = (work - factors[5:6, :] * factors[1:2, :] * before) * factors[6:7, :]
                hopped_kept[t, rows] = final.astype(jnp.bfloat16)
            return carry

        lax.fori_loop(0, per_piece, one_tile, 0)

    def send_down(c, p, copy, copy_self):
        if c == 0:

            @pl.when(p != z)
            def _():
                copy.start()

            @pl.when(p == z)
            def _():
                copy_self()
        else:
            copy.start()

    def down_sent(c, p, copy):
        if c == 0:

            @pl.when(p != z)
            def _():
                copy.wait_send()
        else:
            copy.wait_send()

    def up_range(c):
        return range(c, RING)

    def one_step(c, step, carry):
        for q in range(CHUNKS):
            to_near(q).start()
        if c == 1:
            lend(0).start()
        for part in range(PARTS):
            for p in (2 * c, 2 * c + 1):

                def copy_self(p=p, part=part):
                    gathered[part][down_slot] = own[:, half_rows(p, part)]

                send_down(c, p, own_down(p, part), copy_self)
        tile, count = TILES_OF[c]
        with jax.named_scope("turn_own"):
            for i in range(tile, tile + count):
                if c == 0 and i == tile + count - 1:
                    lend(0).wait_recv()
                turn_tile(c, own, turned, i)
        for part in range(PARTS):
            for k in (2, 1, 3):
                own_up(c, part, k).start()
            if c == 0:
                own_up(c, part, 0).start()
            else:
                gathered[part][pl.ds(up_start + tile, count)] = turned[:count, chip_rows(x, part)]

        @pl.when(step == 0)
        def _():
            with jax.named_scope("diagonal"):
                prepare_diagonal()
            with jax.named_scope("tiles"):
                prepare_tiles()

        @pl.when(step == 1)
        def _():
            sum_middle(0)

        for q in range(CHUNKS + 1):
            if q < CHUNKS:
                with jax.named_scope(f"near{q}"):
                    to_near(q).wait_recv()
                forward(q).start()
                if q == 0 and c == 1:
                    lend(1).start()
            if q >= 1:
                with jax.named_scope(f"far{q - 1}"):
                    forward(q - 1).wait_recv()
                p, part, sub = 2 * c + ((q - 1) // 2) % 2, (q - 1) // 4, (q - 1) % 2

                def copy_self(part=part, sub=sub, q=q):
                    rows = slice(starts[q - 1], starts[q - 1] + sizes[q - 1])
                    gathered[part][late_down_slot, sub * CUTS[0] : sub * CUTS[0] + CUTS[sub]] = far[:, rows]

                send_down(c, p, late_down(p, part, sub), copy_self)
            if q in GROUPS[c]:
                group = GROUPS[c][q]
                for i in range(group[0], group[0] + group[1]):
                    if c == 0 and i == TILES_OF[0][1] - 1:
                        lend(1).wait_recv()
                    turn_tile(c, near, turned_near, i)
                for part in range(PARTS):
                    for k in (2, 1, 3):
                        late_up(c, group, part, k).start()
                    if c == 0:
                        late_up(c, group, part, 0).start()
                    else:
                        gathered[part][pl.ds(late_up_start + group[0], group[1])] = turned_near[
                            group[0] - tile : group[0] - tile + group[1], chip_rows(x, part)
                        ]
            if c == 0 and q == 5:
                with jax.named_scope("arrive0"):
                    arrive(c, 0)
            if c == 0 and q >= 5:
                hop_to(c, 0, ORDER[q - 5])
        if c == 1:
            with jax.named_scope("arrive0"):
                arrive(c, 0)
            for k in ORDER:
                hop_to(c, 0, k)
        with jax.named_scope("arrive1"):
            arrive(c, 1)
        for k in ORDER:
            hop_to(c, 1, k)

        @pl.when(step == 1)
        def _():
            first_numbers()

        for q in range(CHUNKS):
            to_near(q).wait_send()
            forward(q).wait_send()
        if c == 1:
            lend(0).wait_send()
            lend(1).wait_send()
        for part in range(PARTS):
            for p in (2 * c, 2 * c + 1):
                down_sent(c, p, own_down(p, part))
                for sub in range(2):
                    down_sent(c, p, late_down(p, part, sub))
            for k in up_range(c):
                own_up(c, part, k).wait_send()
                for group in GROUPS[c].values():
                    late_up(c, group, part, k).wait_send()

        @pl.when(step == 0)
        def _():
            for to in partners:
                pl.semaphore_signal(free_sem, inc=1, device_id=to, device_id_type=MESH)

        with jax.named_scope("back_up"):
            for part in range(PARTS):
                for k in range(c, RING):
                    result_up(part, k, c).wait_recv()
        with jax.named_scope("turn_back"):
            for t in range(per_piece):
                for i in range(WIDTH):
                    hopped_up[t, i * TILE : (i + 1) * TILE, :] = back_up[i, t * TILE : (t + 1) * TILE, :].T
        with jax.named_scope("back_down"):
            for part in range(PARTS):
                for source in (2 * c, 2 * c + 1):
                    k = (z - source) % RING
                    copy = remote(
                        result.at[part, 0],
                        back_down.at[:, half_rows(source, part)],
                        back_down_send.at[part * RING],
                        back_down_recv.at[part * RING + k],
                        sibling,
                    )
                    if c == 0:

                        @pl.when(source != z)
                        def _():
                            copy.wait_recv()
                    else:
                        copy.wait_recv()
        for part in range(PARTS):
            for k in range(RING):
                if c == 0:
                    if k:
                        result_down(part, k).wait_send()
                    else:

                        @pl.when(z // 2 == 1)
                        def _():
                            result_down(part, 0).wait_send()
                else:
                    result_up(part, k, 0).wait_send()
                    if k:
                        result_up(part, k, 1).wait_send()

        def store_sums(found):
            for i, value in enumerate(found):
                sums[ROWS * i : ROWS * (i + 1), :] = value

        @pl.when(step == 0)
        def _():
            with jax.named_scope("work0"):
                store_sums(each_block(c, first_work))
            sum_start(0)
            with jax.named_scope("free"):
                pl.semaphore_wait(free_sem, len(partners))

        @pl.when(step == 1)
        def _():
            with jax.named_scope("work1"):
                store_sums(each_block(c, second_work))
            sum_start(1)
            with jax.named_scope("sum"):
                sum_middle(1)
                last_numbers()
            with jax.named_scope("finish"):
                finish()

        return carry

    for c in range(2):

        @pl.when(core == c)
        def _(c=c):
            lax.fori_loop(0, STEPS, functools.partial(one_step, c), 0)

    with jax.named_scope("out"):
        stores = []
        for t in range(per_piece):
            copy = pltpu.make_async_copy(
                hopped_kept.at[t], out_ref.at[:, pl.ds(t * TILE, TILE)], load_sem.at[t]
            )
            copy.start()
            stores.append(copy)
        for copy in stores:
            copy.wait()


def body(start_vector, hop_tiles, tile_columns, tile_signs, occupation):
    half, side = start_vector.shape
    tile_k = hop_tiles.shape[1]
    per_piece = side // TILE
    held = RING * per_piece
    quarter = side // RING
    piece = quarter // PARTS
    ups = lax.axis_size("up")
    downs = lax.axis_size("dn")

    anywhere = pl.BlockSpec(memory_space=pl.ANY)
    scalars = pl.BlockSpec(memory_space=pltpu.SMEM)
    vmem = pl.BlockSpec(memory_space=pltpu.VMEM)
    dma = pltpu.SemaphoreType.DMA

    def bf16(*shape):
        return pltpu.VMEM(shape, jnp.bfloat16)

    def f32(*shape):
        return pltpu.VMEM(shape, jnp.float32)

    def pair(*shape):
        return [dma(shape), dma(shape)]

    final, numbers = pl.pallas_call(
        functools.partial(recurrence_kernel, tile_k),
        in_specs=[scalars, anywhere, anywhere, anywhere],
        out_specs=[anywhere, vmem],
        out_shape=[
            jax.ShapeDtypeStruct(start_vector.shape, jnp.bfloat16),
            jax.ShapeDtypeStruct((ROWS, TILE), jnp.float32),
        ],
        scratch_shapes=[
            bf16(per_piece, half + LENT, TILE),
            bf16(per_piece, half + LENT, TILE),
            bf16(per_piece, half, TILE),
            bf16(WIDTH, side, TILE),
            bf16(WIDTH, side, TILE),
            bf16(2 * held, piece, TILE),
            bf16(2 * held, piece, TILE),
            bf16(PARTS, RING, per_piece, piece, TILE),
            bf16(per_piece, half, TILE),
            bf16(WIDTH, side, TILE),
            bf16(per_piece, half + LENT, TILE),
            bf16(held, tile_k, TILE, TILE),
            bf16(per_piece, half, TILE),
            bf16(per_piece, half, TILE),
            pltpu.VMEM(occupation.shape, jnp.int32),
            bf16(per_piece, TILE, TILE),
            bf16(per_piece, TILE, TILE),
            f32(ROWS, TILE),
            f32(3 * ROWS, TILE),
            f32(STEPS, downs, 3 * ROWS, TILE),
            f32(STEPS, ups, 3 * ROWS, TILE),
            f32(ROWS, TILE),
            dma((per_piece,)),
            dma,
            dma,
            *pair(CHUNKS),
            *pair(CHUNKS),
            *pair(2),
            *pair(PARTS * RING),
            *pair(2 * PARTS * RING),
            *pair(2 * PARTS * RING),
            *pair(2 * COUNT * PARTS * RING),
            *pair(PARTS * RING),
            dma((2, PARTS * RING)),
            dma((PARTS * RING,)),
            *pair(STEPS, downs),
            *pair(STEPS, ups),
            pltpu.SemaphoreType.REGULAR,
        ],
        compiler_params=pltpu.CompilerParams(
            collective_id=0, has_side_effects=True, vmem_limit_bytes=67043328
        ),
        name="recurrence",
    )(jnp.concatenate([tile_columns, tile_signs], axis=0), start_vector, hop_tiles, occupation)
    return (final, numbers[0:2, 0], numbers[2:4, 0])


def solution(mesh):
    placed = (P("up", "dn"), P(), P(), P(), P())
    return jax.shard_map(
        body, mesh=mesh, in_specs=placed, out_specs=(P("up", "dn"), P(), P()), check_vma=False
    )
```

```python
import functools

import jax
import jax.numpy as jnp
from jax import lax
from jax.experimental import pallas as pl
from jax.experimental.pallas import tpu as pltpu
from jax.sharding import PartitionSpec as P

STEPS = 2
RING = 4
TILE = 128
MESH = pl.DeviceIdType.MESH

coupling = 4.0


def place():
    u = lax.axis_index("up")
    d = lax.axis_index("dn")
    return u // 8, (u // 2) % 4, u % 2, d // 4, d % 4


def device(y_lo, x, core, y_hi, z):
    return (y_lo * 8 + x * 2 + core, y_hi * 4 + z)


PARTS = 2
CUTS = (112, 96)
CHUNKS = 8
LENT = 64
WIDTH = 7
TILES_OF = ((0, 7), (7, 6))
GROUPS = (
    {1: (0, 1), 3: (1, 2), 5: (3, 1), 6: (4, 1), 7: (5, 2)},
    {1: (7, 1), 3: (8, 1), 5: (9, 2), 6: (11, 1), 7: (12, 1)},
)
COUNT = 5
ROWS = 8
GROUP = 2
EARLY = 5
ORDER = (2, 1, 3, 0)


def recurrence_kernel(
    tile_k,
    lists_ref,
    x_ref,
    tiles_ref,
    occ_ref,
    out_ref,
    numbers_ref,
    own,
    near,
    far,
    turned,
    turned_near,
    gathered_a,
    gathered_b,
    result,
    back_down,
    back_up,
    hopped_up,
    weights,
    kept,
    hopped_kept,
    occ_all,
    occ_rows,
    occ_cols,
    shift_ref,
    sums,
    first,
    second,
    factors,
    load_sem,
    tiles_sem,
    occ_sem,
    near_send,
    near_recv,
    far_send,
    far_recv,
    lend_send,
    lend_recv,
    own_down_send,
    own_down_recv,
    own_up_send,
    own_up_recv,
    late_down_send,
    late_down_recv,
    late_up_send,
    late_up_recv,
    back_down_send,
    back_down_recv,
    back_up_send,
    back_up_recv,
    down_send,
    down_recv,
    up_send,
    up_recv,
    free_sem,
):
    half, side = x_ref.shape
    sites, dets = occ_ref.shape
    quarter = side // RING
    piece = quarter // PARTS
    per_piece = side // TILE
    held = RING * per_piece
    gathered = (gathered_a, gathered_b)
    y_lo, x, core, y_hi, z = place()
    u = lax.axis_index("up")
    d = lax.axis_index("dn")
    ups = lax.axis_size("up")
    downs = lax.axis_size("dn")
    sibling = device(y_lo, x, 1 - core, y_hi, z)
    near_chip = device(1 - y_lo, x, core, y_hi, z)
    far_chip = device(1 - y_lo, x, core, 1 - y_hi, z)

    def remote(src, dst, send, recv, to):
        return pltpu.make_async_remote_copy(
            src_ref=src, dst_ref=dst, send_sem=send, recv_sem=recv, device_id=to, device_id_type=MESH
        )

    starts = [(q // 2) * piece + (q % 2) * CUTS[0] for q in range(CHUNKS)]
    sizes = [CUTS[q % 2] for q in range(CHUNKS)]

    def chip_rows(p, part):
        start = (p // 2) * half + (p % 2) * piece + part * quarter
        return pl.ds(pl.multiple_of(start, 16), piece)

    def half_rows(p, part):
        start = (p % 2) * piece + part * quarter
        return pl.ds(pl.multiple_of(start, 16), piece)

    barrier = pltpu.get_barrier_semaphore()
    partners = [sibling, near_chip, far_chip]
    for k in range(1, RING):
        for c in range(2):
            partners.append(device(y_lo, x, c, y_hi, (z + k) % RING))
            partners.append(device(y_lo, (x + k) % RING, c, y_hi, z))
    others = [device(y_lo, x, core, 1 - y_hi, (z + k) % RING) for k in range(RING)]
    others += [device(1 - y_lo, (x + k) % RING, core, y_hi, z) for k in range(1, RING)]
    others += [device(1 - y_lo, (x + k) % RING, 1 - core, y_hi, z) for k in range(RING)]
    for to in partners + others:
        pl.semaphore_signal(barrier, inc=1, device_id=to, device_id_type=MESH)

    loads = []
    for t in range(per_piece):
        copy = pltpu.make_async_copy(
            x_ref.at[:, pl.ds(t * TILE, TILE)], own.at[t, pl.ds(0, half)], load_sem.at[t]
        )
        copy.start()
        loads.append(copy)
    hop_side = y_hi + core * (y_lo - y_hi)
    first_tile = pl.multiple_of(hop_side * held, held)
    load_tiles = pltpu.make_async_copy(tiles_ref.at[pl.ds(first_tile, held)], weights, tiles_sem)
    load_tiles.start()
    load_occ = pltpu.make_async_copy(occ_ref, occ_all, occ_sem)
    load_occ.start()
    with jax.named_scope("barrier"):
        pl.semaphore_wait(barrier, len(partners) + len(others))
    with jax.named_scope("load"):
        for copy in loads:
            copy.wait()

    down_slot = pl.ds((y_hi * RING + z) * per_piece, per_piece)
    late_down_slot = pl.ds(((1 - y_hi) * RING + z) * per_piece, per_piece)
    up_start = (y_lo * RING + x) * per_piece
    late_up_start = ((1 - y_lo) * RING + x) * per_piece

    def to_near(q):
        rows = pl.ds(starts[q], sizes[q])
        return remote(own.at[:, rows], near.at[:, rows], near_send.at[q], near_recv.at[q], near_chip)

    def forward(q):
        rows = pl.ds(starts[q], sizes[q])
        return remote(near.at[:, rows], far.at[:, rows], far_send.at[q], far_recv.at[q], far_chip)

    def lend(which):
        block = (own, near)[which]
        return remote(
            block.at[:, pl.ds(0, LENT)],
            block.at[:, pl.ds(half, LENT)],
            lend_send.at[which],
            lend_recv.at[which],
            sibling,
        )

    def own_down(p, part):
        at = part * RING + (p - z) % RING
        return remote(
            own.at[:, half_rows(p, part)],
            gathered[part].at[down_slot],
            own_down_send.at[at],
            own_down_recv.at[at],
            device(y_lo, x, 0, y_hi, p),
        )

    def late_down(p, part, sub):
        at = (part * 2 + sub) * RING + (p - z) % RING
        start = (p % 2) * piece + part * quarter + sub * CUTS[0]
        return remote(
            far.at[:, pl.ds(pl.multiple_of(start, 16), CUTS[sub])],
            gathered[part].at[late_down_slot, pl.ds(sub * CUTS[0], CUTS[sub])],
            late_down_send.at[at],
            late_down_recv.at[at],
            device(y_lo, x, 0, y_hi, p),
        )

    def own_up(c, part, k):
        p = (x + k) % RING
        tile, count = TILES_OF[c]
        at = (c * PARTS + part) * RING + k
        return remote(
            turned.at[pl.ds(0, count), chip_rows(p, part)],
            gathered[part].at[pl.ds(up_start + tile, count)],
            own_up_send.at[at],
            own_up_recv.at[at],
            device(y_lo, p, 1, y_hi, z),
        )

    def late_up(c, group, part, k):
        p = (x + k) % RING
        tile, count = group
        number = list(GROUPS[c].values()).index(group)
        at = ((c * COUNT + number) * PARTS + part) * RING + k
        return remote(
            turned_near.at[pl.ds(tile - TILES_OF[c][0], count), chip_rows(p, part)],
            gathered[part].at[pl.ds(late_up_start + tile, count)],
            late_up_send.at[at],
            late_up_recv.at[at],
            device(y_lo, p, 1, y_hi, z),
        )

    def result_down(part, k):
        at = part * RING + k
        return remote(
            result.at[part, k],
            back_down.at[:, half_rows(z, part)],
            back_down_send.at[at],
            back_down_recv.at[at],
            device(y_lo, x, z // 2, y_hi, (z + k) % RING),
        )

    def result_up(part, k, c):
        at = part * RING + k
        return remote(
            result.at[part, k, pl.ds(c * (per_piece - WIDTH), WIDTH)],
            back_up.at[:, chip_rows(x, part)],
            back_up_send.at[c, at],
            back_up_recv.at[at],
            device(y_lo, (x + k) % RING, c, y_hi, z),
        )

    def turn_tile(c, source, target, i):
        top = i * TILE - c * half
        for j in range(per_piece):
            target[i - TILES_OF[c][0], j * TILE : (j + 1) * TILE, :] = source[j, top : top + TILE, :].T

    def hop_piece(part, p, target):
        def one_tile(t):
            i = p * per_piece + t
            picked = [gathered[part][lists_ref[hop_side * held + i, k]] for k in range(tile_k)]
            values = [weights[i, k] for k in range(tile_k)]
            left = jnp.concatenate(picked, axis=1)
            right = jnp.concatenate(values, axis=0)
            return jnp.dot(left, right, preferred_element_type=jnp.float32).astype(jnp.bfloat16)

        def some_tiles(j, carry):
            found = [one_tile(j * GROUP + n) for n in range(GROUP)]
            for n in range(GROUP):
                target[j * GROUP + n] = found[n]
            return carry

        lax.fori_loop(0, per_piece // GROUP, some_tiles, 0)
        for t in range(per_piece // GROUP * GROUP, per_piece):
            target[t] = one_tile(t)

    def hop_to(c, part, k):
        with jax.named_scope(f"hop{part}{k}"):
            if c == 0:
                hop_piece(part, (z + k) % RING, result.at[part, k])
                if k:
                    result_down(part, k).start()
                else:

                    @pl.when(z // 2 == 1)
                    def _():
                        result_down(part, 0).start()

                    @pl.when(z // 2 == 0)
                    def _():
                        back_down[:, half_rows(z, part)] = result[part, 0]
            else:
                hop_piece(part, (x + k) % RING, result.at[part, k])
                result_up(part, k, 0).start()
                if k:
                    result_up(part, k, 1).start()
                else:
                    back_up[:, chip_rows(x, part)] = result[part, 0, per_piece - WIDTH :]

    def arrive(c, part):
        if c == 0:
            for k in range(1, RING):
                own_down((z + k) % RING, part).wait_recv()
                for sub in range(2):
                    late_down((z + k) % RING, part, sub).wait_recv()

            @pl.when(z // 2 == 1)
            def _():
                own_down(z, part).wait_recv()
                for sub in range(2):
                    late_down(z, part, sub).wait_recv()
        else:
            for side_of in range(2):
                for k in range(side_of, RING):
                    own_up(side_of, part, k).wait_recv()
                    for group in GROUPS[side_of].values():
                        late_up(side_of, group, part, k).wait_recv()

    def prepare_tiles():
        load_tiles.wait()

        def one_row(i, carry):
            for k in range(tile_k):
                sign = (1 - 2 * lists_ref[2 * held + hop_side * held + i, k]).astype(jnp.float32)
                weights[i, k] = (weights[i, k].astype(jnp.float32) * sign).astype(jnp.bfloat16).T
            return carry

        lax.fori_loop(0, held, one_row, 0)

    def sum_down(use, j):
        return remote(
            first.at[use, d], first.at[use, d], down_send.at[use, j], down_recv.at[use, j], (u, (d + j) % downs)
        )

    def sum_up(use, j):
        return remote(
            second.at[use, u], second.at[use, u], up_send.at[use, j], up_recv.at[use, j], ((u + j) % ups, d)
        )

    def sum_start(use):
        first[use, d] = sums[...]
        for j in range(1, downs):
            sum_down(use, j).start()

    def sum_middle(use):
        for j in range(1, downs):
            sum_down(use, j).wait()
        total = first[use, 0]
        for j in range(1, downs):
            total = total + first[use, j]
        second[use, u] = total
        for j in range(1, ups):
            sum_up(use, j).start()

    def sum_end(use):
        for j in range(1, ups):
            sum_up(use, j).wait()
        total = second[use, 0]
        for j in range(1, ups):
            total = total + second[use, j]
        parts = [total[ROWS * i : ROWS * (i + 1)] for i in range(3)]
        return [jnp.sum(jnp.sum(part, axis=0, keepdims=True), axis=1, keepdims=True) for part in parts]

    def keep_factor(row, value):
        factors[row : row + 1, :] = jnp.broadcast_to(value, (1, TILE))

    def first_numbers():
        total, cross, square = sum_end(0)
        shift = shift_ref[0:1, 0:1]
        scale = 1.0 / jnp.maximum(jnp.sqrt(total), 1.0)
        alpha = scale * scale * (cross + shift * total)
        delta = alpha - shift
        residual = scale * scale * (square - 2.0 * delta * cross + delta * delta * total)
        beta = jnp.sqrt(jnp.maximum(residual, 1.0))
        keep_factor(0, delta)
        keep_factor(1, scale / beta)
        keep_factor(2, beta * scale)
        keep_factor(3, alpha)
        keep_factor(4, beta)

    def last_numbers():
        total, cross, square = sum_end(1)
        shift = shift_ref[0:1, 0:1]
        alpha = cross + shift * total
        delta = alpha - shift
        residual = square - 2.0 * delta * cross + delta * delta * total
        beta = jnp.sqrt(jnp.maximum(residual, 1.0))
        keep_factor(5, delta)
        keep_factor(6, 1.0 / beta)
        numbers_ref[...] = jnp.zeros_like(numbers_ref)
        numbers_ref[0:1, :] = factors[3:4, :]
        numbers_ref[1:2, :] = jnp.broadcast_to(alpha, (1, TILE))
        numbers_ref[2:3, :] = factors[4:5, :]
        numbers_ref[3:4, :] = jnp.broadcast_to(beta, (1, TILE))

    def prepare_diagonal():
        load_occ.wait()
        blank = jnp.zeros((TILE - sites, TILE), jnp.bfloat16)
        row_base = (y_lo * RING + x) * side
        col_base = d * side

        def one_block(j, carry):
            for base, turn, target in ((row_base, True, occ_rows), (col_base, False, occ_cols)):
                lanes = pl.ds(pl.multiple_of(base + j * TILE, TILE), TILE)
                found = occ_all[:, lanes].astype(jnp.float32).astype(jnp.bfloat16)
                filled = jnp.concatenate([found, blank], axis=0)
                target[j] = filled.T if turn else filled
            return carry

        lax.fori_loop(0, per_piece, one_block, 0)

        def add_tile(j, carry):
            return carry + occ_all[:, pl.ds(pl.multiple_of(j * TILE, TILE), TILE)]

        counts = lax.fori_loop(0, dets // TILE, add_tile, jnp.zeros((sites, TILE), jnp.int32))
        share = jnp.sum(counts.astype(jnp.float32), axis=1, keepdims=True) * (1.0 / dets)
        mean = coupling * jnp.sum(share * share, axis=0, keepdims=True)
        shift_ref[...] = jnp.broadcast_to(mean, shift_ref.shape)

    def fold(value):
        return jnp.sum(value.reshape(-1, ROWS, TILE), axis=0)

    blocks = [(a * TILE, min(TILE, half - a * TILE)) for a in range(WIDTH)]

    def each_block(c, act, late, count=3):
        def one_tile(j, totals):
            t = 3 + j + 2 * (j // 4) if late else j + 4 * (j // 3)
            totals = list(totals)
            for start, size in blocks:
                rows = slice(start, start + size)
                top = c * half + start
                tops = [(top // TILE, top % TILE, min(size, TILE - top % TILE))]
                if tops[0][2] < size:
                    tops.append((top // TILE + 1, 0, size - tops[0][2]))
                left = [occ_rows[i, low : low + n, :] for i, low, n in tops]
                left = left[0] if len(left) == 1 else jnp.concatenate(left, axis=0)
                offset = jnp.dot(left, occ_cols[t], preferred_element_type=jnp.float32)
                offset = coupling * offset - shift_ref[0:1, :]
                lifted = slice(c * LENT + start, c * LENT + start + size)
                found = act(t, rows, lifted, offset)
                if found is not None:
                    totals = [total + fold(value) for total, value in zip(totals, found)]
            return tuple(totals)

        zero = jnp.zeros((ROWS, TILE), jnp.float32)
        return lax.fori_loop(0, per_piece - EARLY if late else EARLY, one_tile, (zero,) * count)

    def both_hops(t, rows, lifted):
        return back_down[t, rows].astype(jnp.float32) + hopped_up[t, lifted].astype(jnp.float32)

    def first_work(t, rows, lifted, offset):
        hopped = both_hops(t, rows, lifted)
        start = own[t, rows]
        kept[t, rows] = start
        hopped_kept[t, rows] = hopped.astype(jnp.bfloat16)
        start = start.astype(jnp.float32)
        work = hopped + offset * start
        own[t, rows] = work.astype(jnp.bfloat16)
        return start * start, work * start, work * work

    def held_vector(t, rows):
        start = kept[t, rows].astype(jnp.float32)
        return start, own[t, rows].astype(jnp.float32) - factors[0:1, :] * start

    def second_work(t, rows, lifted, offset):
        delta, gain, push = factors[0:1, :], factors[1:2, :], factors[2:3, :]
        hopped = both_hops(t, rows, lifted)
        start, before = held_vector(t, rows)
        vector = gain * before
        held_hop = hopped_kept[t, rows].astype(jnp.float32)
        work = gain * (hopped - delta * held_hop + offset * before) - push * start
        high = work.astype(jnp.bfloat16)
        near[t, rows] = high
        far[t, rows] = (work - high.astype(jnp.float32)).astype(jnp.bfloat16)
        return vector * vector, work * vector, work * work

    def store(t):
        return pltpu.make_async_copy(
            hopped_kept.at[t], out_ref.at[:, pl.ds(pl.multiple_of(t * TILE, TILE), TILE)], load_sem.at[t]
        )

    def finish():
        def one_tile(t, carry):
            for start, size in blocks:
                rows = slice(start, start + size)
                work = near[t, rows].astype(jnp.float32) + far[t, rows].astype(jnp.float32)
                _, before = held_vector(t, rows)
                final = (work - factors[5:6, :] * factors[1:2, :] * before) * factors[6:7, :]
                hopped_kept[t, rows] = final.astype(jnp.bfloat16)
            store(t).start()
            return carry

        lax.fori_loop(0, per_piece, one_tile, 0)

    def send_down(c, p, copy, copy_self):
        if c == 0:

            @pl.when(p != z)
            def _():
                copy.start()

            @pl.when(p == z)
            def _():
                copy_self()
        else:
            copy.start()

    def down_sent(c, p, copy):
        if c == 0:

            @pl.when(p != z)
            def _():
                copy.wait_send()
        else:
            copy.wait_send()

    def up_range(c):
        return range(c, RING)

    def one_step(c, step, carry):
        for q in range(CHUNKS):
            to_near(q).start()
        if c == 1:
            lend(0).start()
        for part in range(PARTS):
            for p in (2 * c, 2 * c + 1):

                def copy_self(p=p, part=part):
                    gathered[part][down_slot] = own[:, half_rows(p, part)]

                send_down(c, p, own_down(p, part), copy_self)
        tile, count = TILES_OF[c]
        with jax.named_scope("turn_own"):
            for i in range(tile, tile + count):
                if c == 0 and i == tile + count - 1:
                    lend(0).wait_recv()
                turn_tile(c, own, turned, i)
        for part in range(PARTS):
            for k in (2, 1, 3):
                own_up(c, part, k).start()
            if c == 0:
                own_up(c, part, 0).start()
            else:
                gathered[part][pl.ds(up_start + tile, count)] = turned[:count, chip_rows(x, part)]

        @pl.when(step == 0)
        def _():
            with jax.named_scope("diagonal"):
                prepare_diagonal()
            with jax.named_scope("tiles"):
                prepare_tiles()

        @pl.when(step == 1)
        def _():
            sum_middle(0)

        for q in range(CHUNKS + 1):
            if q < CHUNKS:
                with jax.named_scope(f"near{q}"):
                    to_near(q).wait_recv()
                forward(q).start()
                if q == 0 and c == 1:
                    lend(1).start()
            if q >= 1:
                with jax.named_scope(f"far{q - 1}"):
                    forward(q - 1).wait_recv()
                p, part, sub = 2 * c + ((q - 1) // 2) % 2, (q - 1) // 4, (q - 1) % 2

                def copy_self(part=part, sub=sub, q=q):
                    rows = slice(starts[q - 1], starts[q - 1] + sizes[q - 1])
                    gathered[part][late_down_slot, sub * CUTS[0] : sub * CUTS[0] + CUTS[sub]] = far[:, rows]

                send_down(c, p, late_down(p, part, sub), copy_self)
            if q in GROUPS[c]:
                group = GROUPS[c][q]
                for i in range(group[0], group[0] + group[1]):
                    if c == 0 and i == TILES_OF[0][1] - 1:
                        lend(1).wait_recv()
                    turn_tile(c, near, turned_near, i)
                for part in range(PARTS):
                    for k in (2, 1, 3):
                        late_up(c, group, part, k).start()
                    if c == 0:
                        late_up(c, group, part, 0).start()
                    else:
                        gathered[part][pl.ds(late_up_start + group[0], group[1])] = turned_near[
                            group[0] - tile : group[0] - tile + group[1], chip_rows(x, part)
                        ]
            if c == 0 and q == 5:
                with jax.named_scope("arrive0"):
                    arrive(c, 0)
            if c == 0 and q >= 5:
                hop_to(c, 0, ORDER[q - 5])
        if c == 1:
            with jax.named_scope("arrive0"):
                arrive(c, 0)
            for k in ORDER:
                hop_to(c, 0, k)
        with jax.named_scope("arrive1"):
            arrive(c, 1)
        for k in ORDER:
            hop_to(c, 1, k)

        @pl.when(step == 1)
        def _():
            first_numbers()

        for q in range(CHUNKS):
            to_near(q).wait_send()
            forward(q).wait_send()
        if c == 1:
            lend(0).wait_send()
            lend(1).wait_send()
        for part in range(PARTS):
            for p in (2 * c, 2 * c + 1):
                down_sent(c, p, own_down(p, part))
                for sub in range(2):
                    down_sent(c, p, late_down(p, part, sub))
            for k in up_range(c):
                own_up(c, part, k).wait_send()
                for group in GROUPS[c].values():
                    late_up(c, group, part, k).wait_send()

        @pl.when(step == 0)
        def _():
            for to in partners:
                pl.semaphore_signal(free_sem, inc=1, device_id=to, device_id_type=MESH)

        def take_up(part):
            with jax.named_scope("back_up"):
                for k in range(c, RING):
                    result_up(part, k, c).wait_recv()
            with jax.named_scope("turn_back"):
                for t in (3, 4, 5, 6, 9, 10, 11, 12) if part else (0, 1, 2, 7, 8):
                    for i in range(WIDTH):
                        hopped_up[t, i * TILE : (i + 1) * TILE, :] = back_up[
                            i, t * TILE : (t + 1) * TILE, :
                        ].T

        take_up(0)
        with jax.named_scope("back_down"):
            for part in range(PARTS):
                for source in (2 * c, 2 * c + 1):
                    k = (z - source) % RING
                    copy = remote(
                        result.at[part, 0],
                        back_down.at[:, half_rows(source, part)],
                        back_down_send.at[part * RING],
                        back_down_recv.at[part * RING + k],
                        sibling,
                    )
                    if c == 0:

                        @pl.when(source != z)
                        def _():
                            copy.wait_recv()
                    else:
                        copy.wait_recv()
        def store_sums(found, more):
            for i, value in enumerate(found):
                rows = slice(ROWS * i, ROWS * (i + 1))
                sums[rows, :] = sums[rows, :] + value if more else value

        @pl.when(step == 0)
        def _():
            with jax.named_scope("early0"):
                store_sums(each_block(c, first_work, False), False)

        @pl.when(step == 1)
        def _():
            with jax.named_scope("early1"):
                store_sums(each_block(c, second_work, False), False)

        take_up(1)

        @pl.when(step == 0)
        def _():
            with jax.named_scope("work0"):
                store_sums(each_block(c, first_work, True), True)
            sum_start(0)
            with jax.named_scope("free"):
                pl.semaphore_wait(free_sem, len(partners))

        @pl.when(step == 1)
        def _():
            with jax.named_scope("work1"):
                store_sums(each_block(c, second_work, True), True)
            sum_start(1)
            with jax.named_scope("sum"):
                sum_middle(1)
                last_numbers()
            with jax.named_scope("finish"):
                finish()

        for part in range(PARTS):
            for k in range(RING):
                if c == 0:
                    if k:
                        result_down(part, k).wait_send()
                    else:

                        @pl.when(z // 2 == 1)
                        def _():
                            result_down(part, 0).wait_send()
                else:
                    result_up(part, k, 0).wait_send()
                    if k:
                        result_up(part, k, 1).wait_send()

        return carry

    for c in range(2):

        @pl.when(core == c)
        def _(c=c):
            lax.fori_loop(0, STEPS, functools.partial(one_step, c), 0)

    with jax.named_scope("out"):
        for t in range(per_piece):
            store(t).wait()


def body(start_vector, hop_tiles, tile_columns, tile_signs, occupation):
    half, side = start_vector.shape
    tile_k = hop_tiles.shape[1]
    per_piece = side // TILE
    held = RING * per_piece
    quarter = side // RING
    piece = quarter // PARTS
    ups = lax.axis_size("up")
    downs = lax.axis_size("dn")

    anywhere = pl.BlockSpec(memory_space=pl.ANY)
    scalars = pl.BlockSpec(memory_space=pltpu.SMEM)
    vmem = pl.BlockSpec(memory_space=pltpu.VMEM)
    dma = pltpu.SemaphoreType.DMA

    def bf16(*shape):
        return pltpu.VMEM(shape, jnp.bfloat16)

    def f32(*shape):
        return pltpu.VMEM(shape, jnp.float32)

    def pair(*shape):
        return [dma(shape), dma(shape)]

    final, numbers = pl.pallas_call(
        functools.partial(recurrence_kernel, tile_k),
        in_specs=[scalars, anywhere, anywhere, anywhere],
        out_specs=[anywhere, vmem],
        out_shape=[
            jax.ShapeDtypeStruct(start_vector.shape, jnp.bfloat16),
            jax.ShapeDtypeStruct((ROWS, TILE), jnp.float32),
        ],
        scratch_shapes=[
            bf16(per_piece, half + LENT, TILE),
            bf16(per_piece, half + LENT, TILE),
            bf16(per_piece, half, TILE),
            bf16(WIDTH, side, TILE),
            bf16(WIDTH, side, TILE),
            bf16(2 * held, piece, TILE),
            bf16(2 * held, piece, TILE),
            bf16(PARTS, RING, per_piece, piece, TILE),
            bf16(per_piece, half, TILE),
            bf16(WIDTH, side, TILE),
            bf16(per_piece, half + LENT, TILE),
            bf16(held, tile_k, TILE, TILE),
            bf16(per_piece, half, TILE),
            bf16(per_piece, half, TILE),
            pltpu.VMEM(occupation.shape, jnp.int32),
            bf16(per_piece, TILE, TILE),
            bf16(per_piece, TILE, TILE),
            f32(ROWS, TILE),
            f32(3 * ROWS, TILE),
            f32(STEPS, downs, 3 * ROWS, TILE),
            f32(STEPS, ups, 3 * ROWS, TILE),
            f32(ROWS, TILE),
            dma((per_piece,)),
            dma,
            dma,
            *pair(CHUNKS),
            *pair(CHUNKS),
            *pair(2),
            *pair(PARTS * RING),
            *pair(2 * PARTS * RING),
            *pair(2 * PARTS * RING),
            *pair(2 * COUNT * PARTS * RING),
            *pair(PARTS * RING),
            dma((2, PARTS * RING)),
            dma((PARTS * RING,)),
            *pair(STEPS, downs),
            *pair(STEPS, ups),
            pltpu.SemaphoreType.REGULAR,
        ],
        compiler_params=pltpu.CompilerParams(
            collective_id=0, has_side_effects=True, vmem_limit_bytes=67043328
        ),
        name="recurrence",
    )(jnp.concatenate([tile_columns, tile_signs], axis=0), start_vector, hop_tiles, occupation)
    return (final, numbers[0:2, 0], numbers[2:4, 0])


def solution(mesh):
    placed = (P("up", "dn"), P(), P(), P(), P())
    return jax.shard_map(
        body, mesh=mesh, in_specs=placed, out_specs=(P("up", "dn"), P(), P()), check_vma=False
    )
```
